768 devices in a mesh: gz: 96 (over z, x, core), gy: 8 (over y).
Axes of the slice: x: 4, y: 8, z: 12, core: 2. Of those that a mesh axis runs over, the one named last changes fastest.
Arguments:
- populations: float32 [19, 288, 384, 128], P(None, 'gz', 'gy'), may hold values from 0.1 to 25, as said below
- solute: float32 [7, 288, 384, 128], P(None, 'gz', 'gy'), may hold values from 0.05 to 3, as said below
- pore_mask: int32 [288, 384, 128], P('gz', 'gy'), may hold values from 0 to 2
- mineral_ids: int32 [288, 384, 128], P('gz', 'gy'), may hold values from 0 to 7
- reaction_rates: float32 [8], replicated, may hold values from 0.05 to 0.6
- saturation: float32 [8], replicated, may hold values from 0.5 to 6
Outputs:
- flow_next: float32 [19, 288, 384, 128], P(None, 'gz', 'gy')
- solute_next: float32 [7, 288, 384, 128], P(None, 'gz', 'gy')
The draws below stay inside these ranges and needn't reach their ends.
Inputs may be any that keep to these rules, and one draw needn't show every extreme that they name: `populations`: every population is positive. `solute`: every population is positive.
All inputs are finite; a program needn't handle non-finite values.
Results may differ from the reference program's by a relative error of at most 0.0003.
Values sent between devices are 32-bit elements; how exact they have to be, the bound alone decides.
No kernel may reach another device: no remote copies, remote signals or barrier semaphores. Data moves between devices by JAX's collectives and lax.ppermute only.
A program may use at most 32 MiB of HBM per device.

```python
import math
import jax
import jax.numpy as jnp
import numpy as np
from jax import lax

NX = 128
MINERALS = 8
NZ = 288
NY = 384


LINKS19 = np.array([[0, 0, 0], [1, 0, 0], [-1, 0, 0], [0, 1, 0], [0, -1, 0], [0, 0, 1], [0, 0, -1], [1, 1, 0], [-1, -1, 0], [1, -1, 0], [-1, 1, 0], [1, 0, 1], [-1, 0, -1], [1, 0, -1], [-1, 0, 1], [0, 1, 1], [0, -1, -1], [0, 1, -1], [0, -1, 1]])


WEIGHTS19 = np.array([1.0 / 3.0] + [1.0 / 18.0] * 6 + [1.0 / 36.0] * 12)


WEIGHTS7 = np.array([0.25] + [0.125] * 6)


def draw_populations(key, part):
    key_density, key_velocity, key_jitter = jax.random.split(jax.random.fold_in(key, 11), 3)
    grid_shape = (NZ, NY, NX)
    density_cell = 36.0 * jax.random.uniform(key_density, grid_shape, jnp.float32, 0.8, 1.2)
    velocity_cell = 0.025 * jnp.clip(jax.random.normal(key_velocity, (3,) + grid_shape, jnp.float32), -2.0, 2.0)
    jitter = 0.15 * jnp.clip(jax.random.normal(key_jitter, (19,) + grid_shape, jnp.float32), -2.0, 2.0)
    link_table = jnp.asarray(LINKS19, jnp.float32)
    projected = jnp.tensordot(link_table, velocity_cell, axes=1)
    speed = jnp.sum(velocity_cell * velocity_cell, 0)
    scaled = jnp.asarray(WEIGHTS19, jnp.float32)[:, None, None, None]
    balanced = scaled * density_cell * (1.0 + 3.0 * projected + 4.5 * projected * projected - 1.5 * speed)
    return (balanced * (1.0 + jitter)).astype(jnp.float32)


def draw_solute(key, part):
    key_level, key_jitter = jax.random.split(jax.random.fold_in(key, 23), 2)
    grid_shape = (NZ, NY, NX)
    concentration = jnp.exp(jax.random.uniform(key_level, grid_shape, jnp.float32, 0.0, 2.0794))
    jitter = 0.15 * jnp.clip(jax.random.normal(key_jitter, (7,) + grid_shape, jnp.float32), -2.0, 2.0)
    scaled = jnp.asarray(WEIGHTS7, jnp.float32)[:, None, None, None]
    return (scaled * concentration * (1.0 + jitter)).astype(jnp.float32)


def set_ends(drawn, own_key, least, largest):
    dims = drawn.shape
    index_at = [jax.random.randint(jax.random.fold_in(own_key, axis), (), 0, dims[axis]) for axis in range(len(dims))]
    drawn = drawn.at[tuple(index_at)].set(least)
    longest = dims.index(max(dims))
    index_at[longest] = (index_at[longest] + 1) % dims[longest]
    return drawn.at[tuple(index_at)].set(largest)


def setup_inputs(seed: int = 0) -> dict:
    key_of = jax.random.split(jax.random.key(seed), 7)
    populations = draw_populations(jax.random.fold_in(key_of[6], 71), 0)
    solute = draw_solute(jax.random.fold_in(key_of[6], 71), 0)
    pore_mask = set_ends(jax.random.randint(key_of[2], (NZ, NY, NX), 0, 3), jax.random.fold_in(key_of[2], 1), 0, 2).astype(jnp.int32)
    mineral_ids = set_ends(jax.random.randint(key_of[3], (NZ, NY, NX), 0, MINERALS), jax.random.fold_in(key_of[3], 1), 0, MINERALS - 1).astype(jnp.int32)
    reaction_rates = jnp.clip(jnp.exp(jax.random.uniform(key_of[4], (MINERALS,), jnp.float32, math.log(0.05), math.log(0.6))), 0.05, 0.6)
    saturation = jnp.clip(jax.random.uniform(key_of[5], (MINERALS,), jnp.float32, 0.5, 6.0), 0.5, 6.0)
    return {"populations": populations, "solute": solute, "pore_mask": pore_mask, "mineral_ids": mineral_ids, "reaction_rates": reaction_rates, "saturation": saturation}


LINKS19 = np.array([[0, 0, 0], [1, 0, 0], [-1, 0, 0], [0, 1, 0], [0, -1, 0], [0, 0, 1], [0, 0, -1], [1, 1, 0], [-1, -1, 0], [1, -1, 0], [-1, 1, 0], [1, 0, 1], [-1, 0, -1], [1, 0, -1], [-1, 0, 1], [0, 1, 1], [0, -1, -1], [0, 1, -1], [0, -1, 1]])
REVERSE19 = [0, 2, 1, 4, 3, 6, 5, 8, 7, 10, 9, 12, 11, 14, 13, 16, 15, 18, 17]
WEIGHTS19 = np.array([1.0 / 3.0] + [1.0 / 18.0] * 6 + [1.0 / 36.0] * 12)
WEIGHTS7 = np.array([0.25] + [0.125] * 6)
RELAX_FLOW = 1.25
RELAX_SOLUTE = 1.4


def moment(values, lattice):
    link_table = jnp.asarray(lattice, jnp.float32)
    return jnp.tensordot(link_table.T, values, axes=1, precision=lax.Precision.HIGHEST)


def equilibrium(density, velocity, lattice, weights, linear, quadratic, square_term):
    link_table = jnp.asarray(lattice, jnp.float32)
    projected = jnp.tensordot(link_table, velocity, axes=1, precision=lax.Precision.HIGHEST)
    speed = jnp.sum(velocity * velocity, 0)
    scaled = jnp.asarray(weights, jnp.float32)[:, None, None, None]
    return scaled * density * (1.0 + linear * projected + quadratic * projected * projected - square_term * speed)


def lookup(mineral_ids, values_table):
    kinds = jnp.arange(values_table.shape[0], dtype=jnp.int32)[:, None, None, None]
    return jnp.sum(jnp.where(mineral_ids[None] == kinds, values_table[:, None, None, None], 0.0), 0)


def pull_global(values, shift_z, shift_y, shift_x):
    rolled = jnp.roll(values, shift_z, axis=0)
    if shift_y == 1:
        rolled = jnp.concatenate([jnp.zeros_like(rolled[:, :1]), rolled[:, :-1]], 1)
    elif shift_y == -1:
        rolled = jnp.concatenate([rolled[:, 1:], jnp.zeros_like(rolled[:, :1])], 1)
    return jnp.roll(rolled, shift_x, axis=2)


def stream(relaxed, pore_mask, links_count):
    results = []
    for direction in range(links_count):
        shift_z, shift_y, shift_x = (int(v) for v in LINKS19[direction])
        source = pull_global(pore_mask, shift_z, shift_y, shift_x)
        arrived = pull_global(relaxed[direction], shift_z, shift_y, shift_x)
        results.append(jnp.where(source == 0, relaxed[REVERSE19[direction]], arrived))
    return jnp.stack(results)


def reference(populations, solute, pore_mask, mineral_ids, reaction_rates, saturation):
    density = jnp.sum(populations, 0)
    velocity = moment(populations, LINKS19) / density
    balanced = equilibrium(density, velocity, LINKS19, WEIGHTS19, 3.0, 4.5, 1.5)
    relaxed = populations - (populations - balanced) / RELAX_FLOW
    flow_next = jnp.where(pore_mask[None] == 0, populations, stream(relaxed, pore_mask, 19))
    density_next = jnp.sum(flow_next, 0)
    velocity_next = jnp.where(pore_mask[None] > 0, moment(flow_next, LINKS19) / density_next, 0.0)
    concentration = jnp.sum(solute, 0)
    rate_cell = lookup(mineral_ids, reaction_rates)
    target = lookup(mineral_ids, saturation)
    reaction = jnp.where(pore_mask == 2, -rate_cell * (concentration - target), 0.0)
    solute_balanced = equilibrium(concentration, velocity_next, LINKS19[:7], WEIGHTS7, 4.0, 0.0, 0.0)
    weights = jnp.asarray(WEIGHTS7, jnp.float32)[:, None, None, None]
    solute_relaxed = solute - (solute - solute_balanced) / RELAX_SOLUTE + weights * reaction
    solute_next = jnp.where(pore_mask[None] == 0, solute, stream(solute_relaxed, pore_mask, 7))
    return flow_next, solute_next
```

```python
import functools

import jax
import jax.numpy as jnp
import numpy as np
from jax import lax
from jax.experimental import pallas as pl
from jax.experimental.pallas import tpu as pltpu
from jax.sharding import PartitionSpec as P

LINKS = (
    (0, 0, 0),
    (1, 0, 0),
    (-1, 0, 0),
    (0, 1, 0),
    (0, -1, 0),
    (0, 0, 1),
    (0, 0, -1),
    (1, 1, 0),
    (-1, -1, 0),
    (1, -1, 0),
    (-1, 1, 0),
    (1, 0, 1),
    (-1, 0, -1),
    (1, 0, -1),
    (-1, 0, 1),
    (0, 1, 1),
    (0, -1, -1),
    (0, 1, -1),
    (0, -1, 1),
)
REVERSE = (0, 2, 1, 4, 3, 6, 5, 8, 7, 10, 9, 12, 11, 14, 13, 16, 15, 18, 17)
W19 = (1.0 / 3.0,) + (1.0 / 18.0,) * 6 + (1.0 / 36.0,) * 12
W7 = (0.25,) + (0.125,) * 6
UP = tuple(q for q in range(19) if LINKS[q][0] == 1)
DOWN = tuple(q for q in range(19) if LINKS[q][0] == -1)
KEEP = 1.0 - 1.0 / 1.25
GAIN = 1.0 / 1.25
KEEP_S = 1.0 - 1.0 / 1.4
GAIN_S = 1.0 / 1.4
LX = 128
PAD = 8
MAX_VMEM = 16 * 1024 * 1024


def relax(p):
    d = {q: p[q] - p[q + 1] for q in range(1, 19, 2)}
    s = {q: p[q] + p[q + 1] for q in range(1, 19, 2)}
    density = p[0] + (
        ((s[1] + s[3]) + (s[5] + s[7])) + ((s[9] + s[11]) + (s[13] + s[15])) + s[17]
    )
    mz = (d[1] + d[7]) + (d[9] + d[11]) + d[13]
    my = (d[3] + d[7]) + (d[15] + d[17]) - d[9]
    mx = (d[5] + d[11]) + (d[15] - d[13]) - d[17]
    inverse = 1.0 / density
    uz, uy, ux = mz * inverse, my * inverse, mx * inverse
    rest = 1.0 - 1.5 * (uz * uz + uy * uy + ux * ux)
    out = [None] * 19
    scaled = {w: density * (GAIN * w) for w in set(W19)}
    out[0] = KEEP * p[0] + scaled[W19[0]] * rest
    along = {
        1: uz,
        3: uy,
        5: ux,
        7: uz + uy,
        9: uz - uy,
        11: uz + ux,
        13: uz - ux,
        15: uy + ux,
        17: uy - ux,
    }
    for q, e in along.items():
        w = scaled[W19[q]]
        even = w * (rest + 4.5 * (e * e))
        odd = w * (3.0 * e)
        out[q] = KEEP * p[q] + (even + odd)
        out[q + 1] = KEEP * p[q + 1] + (even - odd)
    return out


def solute_terms(s, pore, ids, rates_ref, target_ref):
    total = ((s[0] + s[1]) + (s[2] + s[3])) + ((s[4] + s[5]) + s[6])
    rate = jnp.full(total.shape, rates_ref[0], jnp.float32)
    target = jnp.full(total.shape, target_ref[0], jnp.float32)
    for k in range(1, rates_ref.shape[0]):
        rate = jnp.where(ids == k, rates_ref[k], rate)
        target = jnp.where(ids == k, target_ref[k], target)
    reaction = jnp.where(pore == 2, -rate * (total - target), 0.0)
    return total, reaction


def rolled(value, shift):
    return value if shift == 0 else pltpu.roll(value, shift % LX, axis=1)


def pack_edges(pop, sol, pore, ids, rates, target, up, down):
    width = pop.shape[2]
    for out, first, link, near in ((up, width - 2, 3, 1), (down, 0, 4, 0)):
        rows = slice(first, first + 2)
        for layer in range(3):
            into = slice(2 * layer, 2 * layer + 2)
            for q in range(19):
                out[q, into, :] = pop[q, layer, rows, :]
            kind = pore[layer, rows, :]
            out[19, into, :] = jnp.where(kind > 0, 1.0, 0.0)
            s = [sol[q, layer, rows, :] for q in range(7)]
            total, reaction = solute_terms(s, kind, ids[layer, rows, :], rates, target)
            w = W7[link]
            out[20, into, :] = KEEP_S * s[link] + (w * GAIN_S) * total + w * reaction
            out[21, into, :] = (4.0 * w * GAIN_S) * total
        out[:, 6:8, :] = jnp.zeros((22, 2, LX), jnp.float32)


def streamed(q, layer, row, count, shifted, plain, masks):
    ez, ey, ex = LINKS[q]
    value = shifted(q, layer - ez, row - ey, count)
    if q == 0:
        return value
    open_ = masks(ex, layer - ez, row - ey, count) > 0.0
    return jnp.where(open_, value, plain(REVERSE[q], layer, row, count))


def relax_kernel(
    pop, sol, pore, ids, rates, target, low, high, moved, kept, mask, up, down, edge
):
    width = pop.shape[2]
    tiles = width // 8
    for layer in range(3):
        for t in range(tiles):
            rows, into = slice(8 * t, 8 * t + 8), slice(PAD + 8 * t, PAD + 8 * t + 8)
            out = relax([pop[q, layer, rows, :] for q in range(19)])
            for q in range(19):
                ex = LINKS[q][2]
                moved[q, layer, into, :] = rolled(out[q], ex)
                if ex:
                    kept[q, layer, into, :] = out[q]
            m = jnp.where(pore[layer, rows, :] > 0, 1.0, 0.0)
            for ex in (0, 1, -1):
                mask[ex % 3, layer, into, :] = rolled(m, ex)
    for ref, at in ((low, PAD - 2), (high, PAD + width)):
        p = [ref[q] for q in range(19)]
        m = ref[19]
        p[0] = jnp.where(m > 0.0, p[0], p[0] + 1.0)
        out = relax(p)
        into = slice(at, at + 2)
        for q in range(19):
            ex = LINKS[q][2]
            edge[0, q] = rolled(out[q], ex)
            if ex:
                edge[1, q] = out[q]
        for ex in (0, 1, -1):
            edge[2, ex % 3] = rolled(m, ex)
        for layer in range(3):
            rows = slice(2 * layer, 2 * layer + 2)
            for q in range(19):
                moved[q, layer, into, :] = edge[0, q, rows, :]
                if LINKS[q][2]:
                    kept[q, layer, into, :] = edge[1, q, rows, :]
            for k in range(3):
                mask[k, layer, into, :] = edge[2, k, rows, :]

    def shifted(q, layer, row, count):
        return moved[q, layer, row : row + count, :]

    def plain(q, layer, row, count):
        return (kept if LINKS[q][2] else moved)[q, layer, row : row + count, :]

    def masks(ex, layer, row, count):
        return mask[ex % 3, layer, row : row + count, :]

    for out, layer, sign, cross, link in ((up, 2, 1, UP, 1), (down, 0, -1, DOWN, 2)):
        w = W7[link]
        for t in range(tiles):
            row = PAD + 8 * t
            get = functools.partial(
                streamed, layer=layer, row=row, count=8, shifted=shifted, plain=plain, masks=masks
            )
            away = functools.reduce(jnp.add, [get(q) for q in cross])
            level = functools.reduce(
                jnp.add, [get(q) for q in range(19) if LINKS[q][0] == 0]
            )
            partial = level + away
            rows = slice(8 * t, 8 * t + 8)
            s = [sol[q, layer, rows, :] for q in range(7)]
            total, reaction = solute_terms(
                s, pore[layer, rows, :], ids[layer, rows, :], rates, target
            )
            slope = (4.0 * w * GAIN_S) * total
            base = KEEP_S * s[link] + (w * GAIN_S) * total + w * reaction
            for k, q in enumerate(cross):
                out[k * width + 8 * t : k * width + 8 * t + 8, :] = plain(q, layer, row, 8)
            fields = (masks(0, layer, row, 8), base - slope, partial, slope * (partial + away))
            for k, v in enumerate(fields):
                at = (5 + k) * width + 8 * t
                out[at : at + 8, :] = v
        for k in range(6):
            for side, row in ((0, PAD - 2), (1, PAD + width)):
                at = 9 * width + 4 * k + 2 * side
                v = plain(cross[k], layer, row, 2) if k < 5 else masks(0, layer, row, 2)
                out[at : at + 2, :] = v


def stream_kernel(
    pop,
    sol,
    pore,
    ids,
    rates,
    target,
    low,
    high,
    moved,
    kept,
    mask,
    below,
    above,
    flow,
    solute,
    zmoved,
    zkept,
    zmask,
    plain_s,
    moved_s,
    cross_s,
):
    width = pop.shape[2]
    tiles = width // 8
    sides = ((0, below, UP), (1, above, DOWN))
    for side, ref, links in sides:
        for k in range(6):
            for lo, at in ((0, PAD - 2), (1, PAD + width)):
                src = 9 * width + 4 * k + 2 * lo
                v = ref[src : src + 2, :]
                if k < 5:
                    ex = LINKS[links[k]][2]
                    zmoved[side, k, at : at + 2, :] = rolled(v, ex)
                    if ex:
                        zkept[side, k, at : at + 2, :] = v
                else:
                    for ex in (0, 1, -1):
                        zmask[side, ex % 3, at : at + 2, :] = rolled(v, ex)
            for t in range(tiles):
                at = PAD + 8 * t
                v = ref[k * width + 8 * t : k * width + 8 * t + 8, :]
                if k < 5:
                    ex = LINKS[links[k]][2]
                    zmoved[side, k, at : at + 8, :] = rolled(v, ex)
                    if ex:
                        zkept[side, k, at : at + 8, :] = v
                else:
                    for ex in (0, 1, -1):
                        zmask[side, ex % 3, at : at + 8, :] = rolled(v, ex)

    def shifted(q, layer, row, count):
        if layer == -1:
            return zmoved[0, UP.index(q), row : row + count, :]
        if layer == 3:
            return zmoved[1, DOWN.index(q), row : row + count, :]
        return moved[q, layer, row : row + count, :]

    def plain(q, layer, row, count):
        if layer == -1:
            ref, k = (zkept if LINKS[q][2] else zmoved), UP.index(q)
            return ref[0, k, row : row + count, :]
        if layer == 3:
            ref, k = (zkept if LINKS[q][2] else zmoved), DOWN.index(q)
            return ref[1, k, row : row + count, :]
        return (kept if LINKS[q][2] else moved)[q, layer, row : row + count, :]

    def masks(ex, layer, row, count):
        if layer == -1:
            return zmask[0, ex % 3, row : row + count, :]
        if layer == 3:
            return zmask[1, ex % 3, row : row + count, :]
        return mask[ex % 3, layer, row : row + count, :]

    def sums(f):
        d = {q: f[q] - f[q + 1] for q in range(1, 19, 2)}
        s = {q: f[q] + f[q + 1] for q in range(1, 19, 2)}
        density = f[0] + (
            ((s[1] + s[3]) + (s[5] + s[7])) + ((s[9] + s[11]) + (s[13] + s[15])) + s[17]
        )
        mz = (d[1] + d[7]) + (d[9] + d[11]) + d[13]
        my = (d[3] + d[7]) + (d[15] + d[17]) - d[9]
        mx = (d[5] + d[11]) + (d[15] - d[13]) - d[17]
        return density, mz, my, mx

    def pull(layer, row, count):
        return [
            streamed(q, layer, row, count, shifted, plain, masks) for q in range(19)
        ]

    for side, ref, layer, links in ((0, below, 0, DOWN), (1, above, 2, UP)):
        outside = -1 if side == 0 else 3
        for t in range(tiles):
            row = PAD + 8 * t
            into = functools.reduce(
                jnp.add,
                [streamed(q, outside, row, 8, shifted, plain, masks) for q in links],
            )
            base, partial, weight = (
                ref[(6 + k) * width + 8 * t : (6 + k) * width + 8 * t + 8, :] for k in range(3)
            )
            cross_s[side, 8 * t : 8 * t + 8, :] = base + weight / (partial + into)
    for layer in range(3):
        for ref, row, near, link, sign, part in (
            (low, PAD - 1, 1, 3, 1.0, 1),
            (high, PAD + width, 0, 4, -1.0, 0),
        ):
            density, _, my, _ = sums(pull(layer, row, 1))
            at = 2 * layer + near
            plain_s[link, layer, row : row + 1, :] = ref[20, at : at + 1, :] + sign * (
                ref[21, at : at + 1, :] * (my / density)
            )
        for t in range(tiles):
            row, rows = PAD + 8 * t, slice(8 * t, 8 * t + 8)
            f = pull(layer, row, 8)
            kind = pore[layer, rows, :]
            rock = kind == 0
            for q in range(19):
                flow[q, layer, rows, :] = jnp.where(rock, pop[q, layer, rows, :], f[q])
            density, mz, my, mx = sums(f)
            inverse = jnp.where(rock, 0.0, 1.0 / density)
            s = [sol[q, layer, rows, :] for q in range(7)]
            total, reaction = solute_terms(s, kind, ids[layer, rows, :], rates, target)
            side_term = (W7[1] * GAIN_S) * total + W7[1] * reaction
            slope = (4.0 * W7[1] * GAIN_S) * total * inverse
            into = slice(row, row + 8)
            plain_s[0, layer, into, :] = (
                KEEP_S * s[0] + (W7[0] * GAIN_S) * total + W7[0] * reaction
            )
            for q, m in ((1, mz), (3, my), (5, mx)):
                plain_s[q, layer, into, :] = KEEP_S * s[q] + side_term + slope * m
                plain_s[q + 1, layer, into, :] = KEEP_S * s[q + 1] + side_term - slope * m
            for q in (5, 6):
                ex = LINKS[q][2]
                moved_s[q - 5, layer, into, :] = rolled(plain_s[q, layer, into, :], ex)
    for layer in range(3):
        for t in range(tiles):
            row, rows = PAD + 8 * t, slice(8 * t, 8 * t + 8)
            rock = pore[layer, rows, :] == 0
            for q in range(7):
                ez, ey, ex = LINKS[q]
                src = layer - ez
                if q == 0:
                    value = plain_s[0, layer, row : row + 8, :]
                else:
                    if src == -1:
                        value = cross_s[0, rows, :]
                    elif src == 3:
                        value = cross_s[1, rows, :]
                    elif ex:
                        value = moved_s[q - 5, layer, row : row + 8, :]
                    else:
                        value = plain_s[q, src, row - ey : row - ey + 8, :]
                    open_ = masks(ex, src, row - ey, 8) > 0.0
                    value = jnp.where(open_, value, plain_s[REVERSE[q], layer, row : row + 8, :])
                solute[q, layer, rows, :] = jnp.where(rock, sol[q, layer, rows, :], value)


VMEM = pl.BlockSpec(memory_space=pltpu.VMEM)
SMEM = pl.BlockSpec(memory_space=pltpu.SMEM)


def call(kernel, operands, specs, outs, scratch=(), flops=1_000_000):
    return pl.pallas_call(
        kernel,
        out_shape=[jax.ShapeDtypeStruct(s, jnp.float32) for s in outs],
        in_specs=list(specs),
        out_specs=[VMEM] * len(outs),
        scratch_shapes=[pltpu.VMEM(s, jnp.float32) for s in scratch],
        compiler_params=pltpu.CompilerParams(vmem_limit_bytes=MAX_VMEM),
        cost_estimate=pl.CostEstimate(flops=flops, bytes_accessed=1_000_000, transcendentals=0),
    )(*operands)


def on_device(populations, solute, pore_mask, mineral_ids, reaction_rates, saturation):
    width = pore_mask.shape[1]
    padded = width + 2 * PAD
    cells = (populations, solute, pore_mask, mineral_ids, reaction_rates, saturation)
    kinds = [VMEM] * 4 + [SMEM] * 2
    gz, gy = lax.axis_size("gz"), lax.axis_size("gy")
    edges = call(pack_edges, cells, kinds, [(22, 8, LX)] * 2)
    low = lax.ppermute(edges[0], "gy", [(i, i + 1) for i in range(gy - 1)])
    high = lax.ppermute(edges[1], "gy", [(i + 1, i) for i in range(gy - 1)])
    rows = 9 * width + 24
    moved, kept, mask, up, down = call(
        relax_kernel,
        cells + (low, high),
        kinds + [VMEM] * 2,
        [(19, 3, padded, LX), (19, 3, padded, LX), (3, 3, padded, LX), (rows, LX), (rows, LX)],
        [(3, 19, 8, LX)],
    )
    below = lax.ppermute(up, "gz", [(i, (i + 1) % gz) for i in range(gz)])
    above = lax.ppermute(down, "gz", [((i + 1) % gz, i) for i in range(gz)])
    return tuple(
        call(
            stream_kernel,
            cells + (low, high, moved, kept, mask, below, above),
            kinds + [VMEM] * 7,
            [populations.shape, solute.shape],
            [
                (2, 5, padded, LX),
                (2, 5, padded, LX),
                (2, 3, padded, LX),
                (7, 3, padded, LX),
                (2, 3, padded, LX),
                (2, width, LX),
            ],
        )
    )


def solution(mesh):
    cells = P(None, "gz", "gy", None)
    return jax.shard_map(
        on_device,
        mesh=mesh,
        in_specs=(cells, cells, P("gz", "gy", None), P("gz", "gy", None), P(), P()),
        out_specs=(cells, cells),
        check_vma=False,
    )
```

```python
import functools

import jax
import jax.numpy as jnp
import numpy as np
from jax import lax
from jax.experimental import pallas as pl
from jax.experimental.pallas import tpu as pltpu
from jax.sharding import PartitionSpec as P

LINKS = (
    (0, 0, 0),
    (1, 0, 0),
    (-1, 0, 0),
    (0, 1, 0),
    (0, -1, 0),
    (0, 0, 1),
    (0, 0, -1),
    (1, 1, 0),
    (-1, -1, 0),
    (1, -1, 0),
    (-1, 1, 0),
    (1, 0, 1),
    (-1, 0, -1),
    (1, 0, -1),
    (-1, 0, 1),
    (0, 1, 1),
    (0, -1, -1),
    (0, 1, -1),
    (0, -1, 1),
)
REVERSE = (0, 2, 1, 4, 3, 6, 5, 8, 7, 10, 9, 12, 11, 14, 13, 16, 15, 18, 17)
W19 = (1.0 / 3.0,) + (1.0 / 18.0,) * 6 + (1.0 / 36.0,) * 12
W7 = (0.25,) + (0.125,) * 6
UP = tuple(q for q in range(19) if LINKS[q][0] == 1)
DOWN = tuple(q for q in range(19) if LINKS[q][0] == -1)
KEEP = 1.0 - 1.0 / 1.25
GAIN = 1.0 / 1.25
KEEP_S = 1.0 - 1.0 / 1.4
GAIN_S = 1.0 / 1.4
LX = 128
PAD = 8
MAX_VMEM = 12 * 1024 * 1024
NEAR = 23
FAR_ROWS = 3 * NEAR
EDGE_ROWS = 88
SPAN = 4


def relax(p):
    d = {q: p[q] - p[q + 1] for q in range(1, 19, 2)}
    s = {q: p[q] + p[q + 1] for q in range(1, 19, 2)}
    density = p[0] + (
        ((s[1] + s[3]) + (s[5] + s[7])) + ((s[9] + s[11]) + (s[13] + s[15])) + s[17]
    )
    mz = (d[1] + d[7]) + (d[9] + d[11]) + d[13]
    my = (d[3] + d[7]) + (d[15] + d[17]) - d[9]
    mx = (d[5] + d[11]) + (d[15] - d[13]) - d[17]
    inverse = 1.0 / density
    uz, uy, ux = mz * inverse, my * inverse, mx * inverse
    rest = 1.0 - 1.5 * (uz * uz + uy * uy + ux * ux)
    out = [None] * 19
    scaled = {w: density * (GAIN * w) for w in set(W19)}
    out[0] = KEEP * p[0] + scaled[W19[0]] * rest
    along = {
        1: uz,
        3: uy,
        5: ux,
        7: uz + uy,
        9: uz - uy,
        11: uz + ux,
        13: uz - ux,
        15: uy + ux,
        17: uy - ux,
    }
    for q, e in along.items():
        w = scaled[W19[q]]
        even = w * (rest + 4.5 * (e * e))
        odd = w * (3.0 * e)
        out[q] = KEEP * p[q] + (even + odd)
        out[q + 1] = KEEP * p[q + 1] + (even - odd)
    return out


def solute_terms(s, pore, ids, rates_ref, target_ref):
    total = ((s[0] + s[1]) + (s[2] + s[3])) + ((s[4] + s[5]) + s[6])
    rate = jnp.full(total.shape, rates_ref[0], jnp.float32)
    target = jnp.full(total.shape, target_ref[0], jnp.float32)
    for k in range(1, rates_ref.shape[0]):
        rate = jnp.where(ids == k, rates_ref[k], rate)
        target = jnp.where(ids == k, target_ref[k], target)
    reaction = jnp.where(pore == 2, -rate * (total - target), 0.0)
    return total, reaction


def rolled(value, shift):
    return value if shift == 0 else pltpu.roll(value, shift % LX, axis=1)


def sums(f):
    d = {q: f[q] - f[q + 1] for q in range(1, 19, 2)}
    s = {q: f[q] + f[q + 1] for q in range(1, 19, 2)}
    density = f[0] + (
        ((s[1] + s[3]) + (s[5] + s[7])) + ((s[9] + s[11]) + (s[13] + s[15])) + s[17]
    )
    mz = (d[1] + d[7]) + (d[9] + d[11]) + d[13]
    my = (d[3] + d[7]) + (d[15] + d[17]) - d[9]
    mx = (d[5] + d[11]) + (d[15] - d[13]) - d[17]
    return density, mz, my, mx


def add_all(values):
    values = list(values)
    while len(values) > 1:
        values = [
            values[i] + values[i + 1] if i + 1 < len(values) else values[i]
            for i in range(0, len(values), 2)
        ]
    return values[0]


def toward(sign):
    return tuple(q for q in range(19) if LINKS[q][1] == sign)


def pack_edges(pop, sol, pore, ids, up, down, epop, esol, epore, eids, erel, sems):
    width = pop.shape[2]
    copies = []
    for side, first in ((0, width - 8), (1, 0)):
        rows = pl.ds(first, 8)
        for k, (src, dst) in enumerate(
            (
                (pop.at[:, :, rows, :], epop),
                (sol.at[:, :, rows, :], esol),
                (pore.at[:, rows, :], epore),
                (ids.at[:, rows, :], eids),
            )
        ):
            copy = pltpu.make_async_copy(src, dst.at[side], sems.at[side, k])
            copy.start()
            copies.append(copy)
    for copy in copies:
        copy.wait()
    for side, out, near, far, link, sign in ((0, up, 7, 6, 3, 1), (1, down, 0, 1, 4, -1)):
        for layer in range(3):
            rel = relax([epop[side, q, layer] for q in range(19)])
            for q in range(19):
                erel[side, layer, q] = rel[q]
            kind = epore[side, layer].astype(jnp.float32)
            erel[side, layer, 19] = kind
            erel[side, layer, 20] = eids[side, layer].astype(jnp.float32)
            erel[side, layer, 21] = add_all(esol[side, q, layer] for q in range(7))
            erel[side, layer, 22] = esol[side, link, layer]
        for layer in range(3):
            for k in range(NEAR):
                at = 3 * k + layer
                out[at : at + 1, :] = erel[side, layer, k, near : near + 1, :]
            for k, q in enumerate(toward(sign) + (19,)):
                at = FAR_ROWS + 3 * k + layer
                out[at : at + 1, :] = erel[side, layer, q, far : far + 1, :]
        out[EDGE_ROWS - 1 : EDGE_ROWS, :] = jnp.zeros((1, LX), jnp.float32)


def relax_kernel(pop, sol, pore, ids, rates, target, moved, kept, mask, chem):
    width = pop.shape[2]
    for layer in range(3):
        for t in range(width // 8):
            rows, into = slice(8 * t, 8 * t + 8), slice(PAD + 8 * t, PAD + 8 * t + 8)
            out = relax([pop[q, layer, rows, :] for q in range(19)])
            for q in range(19):
                ex = LINKS[q][2]
                moved[q, layer, into, :] = rolled(out[q], ex)
                if ex:
                    kept[q, layer, into, :] = out[q]
            kind = pore[layer, rows, :]
            m = jnp.where(kind > 0, 1.0, 0.0)
            for ex in (0, 1, -1):
                mask[ex % 3, layer, into, :] = rolled(m, ex)
            s = [sol[q, layer, rows, :] for q in range(7)]
            total, reaction = solute_terms(s, kind, ids[layer, rows, :], rates, target)
            chem[0, layer, rows, :] = total
            chem[1, layer, rows, :] = reaction


def streamed(q, layer, row, count, shifted, plain, masks):
    ez, ey, ex = LINKS[q]
    value = shifted(q, layer - ez, row - ey, count)
    if q == 0:
        return value
    open_ = masks(ex, layer - ez, row - ey, count) > 0.0
    return jnp.where(open_, value, plain(REVERSE[q], layer, row, count))


def readers(moved, kept, mask):
    def shifted(q, layer, row, count):
        return moved[q, layer, row : row + count, :]

    def plain(q, layer, row, count):
        return (kept if LINKS[q][2] else moved)[q, layer, row : row + count, :]

    def masks(ex, layer, row, count):
        return mask[ex % 3, layer, row : row + count, :]

    return shifted, plain, masks


def by_parity(body, first, second):
    odd = lax.rem(lax.axis_index("gz"), 2)

    @pl.when(odd == 0)
    def _():
        body(first, second)

    @pl.when(odd == 1)
    def _():
        body(second, first)


def face_kernel(
    moved_in, kept_in, mask_in, low, high, sol, chem, moved, kept, mask, across, on_chip, turned
):
    del moved_in, kept_in, mask_in
    width = sol.shape[2]
    for side, ref, near, far, sign in (
        (0, low, PAD - 1, PAD - 2, 1),
        (1, high, PAD + width, PAD + width + 1, -1),
    ):
        for t in range(EDGE_ROWS // 8):
            v = ref[8 * t : 8 * t + 8, :]
            turned[side, 0, 8 * t : 8 * t + 8, :] = rolled(v, 1)
            turned[side, 1, 8 * t : 8 * t + 8, :] = rolled(v, -1)

        def line(at, ex):
            if ex == 0:
                return ref[at : at + 1, :]
            return turned[side, 0 if ex == 1 else 1, at : at + 1, :]

        for layer in range(3):
            for row, start, links in (
                (near, 0, tuple(range(19))),
                (far, FAR_ROWS, toward(sign)),
            ):
                into = slice(row, row + 1)
                for k, q in enumerate(links):
                    at, ex = start + 3 * k + layer, LINKS[q][2]
                    moved[q, layer, into, :] = line(at, ex)
                    if ex:
                        kept[q, layer, into, :] = line(at, 0)
                at = start + 3 * len(links) + layer
                for ex in (0, 1, -1):
                    mask[ex % 3, layer, into, :] = line(at, ex)
    shifted, plain, masks = readers(moved, kept, mask)

    def emit(up, down):
        span = width + SPAN
        for out, layer, cross, link in ((up, 2, UP, 1), (down, 0, DOWN, 2)):
            w = W7[link]
            for t in range(width // 8):
                row, rows = PAD + 8 * t, slice(8 * t, 8 * t + 8)
                get = functools.partial(
                    streamed,
                    layer=layer,
                    row=row,
                    count=8,
                    shifted=shifted,
                    plain=plain,
                    masks=masks,
                )
                away = add_all(get(q) for q in cross)
                level = add_all(get(q) for q in range(19) if LINKS[q][0] == 0)
                partial = level + away
                total, reaction = chem[0, layer, rows, :], chem[1, layer, rows, :]
                slope = (4.0 * w * GAIN_S) * total
                base = KEEP_S * sol[link, layer, rows, :] + (w * GAIN_S) * total + w * reaction
                for k, v in enumerate((base - slope, partial, slope * (partial + away))):
                    at = 6 * span + k * width + 8 * t
                    out[at : at + 8, :] = v
            for k in range(6):
                at = k * span
                pieces = [(PAD - 2, 2, 0)]
                pieces += [(PAD + 8 * t, 8, 2 + 8 * t) for t in range(width // 8)]
                pieces += [(PAD + width, 2, 2 + width)]
                for row, count, to in pieces:
                    v = plain(cross[k], layer, row, count) if k < 5 else masks(0, layer, row, count)
                    out[at + to : at + to + count, :] = v

    by_parity(emit, on_chip, across)


def inner_kernel(
    pop,
    sol,
    pore,
    chem,
    moved,
    kept,
    mask,
    low,
    high,
    rates,
    target,
    flow,
    part,
    edge_part,
    edge_chem,
    middle,
    middle_moved,
    buffer,
    sems,
):
    width = pop.shape[2]
    tiles = width // 8
    shifted, plain, masks = readers(moved, kept, mask)
    zero8 = jnp.zeros((8, LX), jnp.float32)
    zero1 = jnp.zeros((1, LX), jnp.float32)

    def pull(layer, row, count, zero):
        return [
            streamed(q, layer, row, count, shifted, plain, masks)
            if 0 <= layer - LINKS[q][0] <= 2
            else zero
            for q in range(19)
        ]

    copies = []
    for layer in (1, 0, 2):
        for t in range(tiles):
            row, rows = PAD + 8 * t, slice(8 * t, 8 * t + 8)
            f = pull(layer, row, 8, zero8)
            rock = pore[layer, rows, :] == 0
            for q in range(19):
                if 0 <= layer - LINKS[q][0] <= 2:
                    buffer[q, layer, rows, :] = jnp.where(rock, pop[q, layer, rows, :], f[q])
            density, mz, my, mx = sums(f)
            if layer != 1:
                for k, v in enumerate((density, mz, my, mx)):
                    part[layer // 2, k, rows, :] = v
                continue
            relaxed = relax_solute(
                [sol[q, layer, rows, :] for q in range(7)],
                chem[0, layer, rows, :],
                chem[1, layer, rows, :],
                jnp.where(rock, 0.0, 1.0 / density),
                (mz, my, mx),
            )
            into = slice(row, row + 8)
            for q in range(7):
                middle[q, into, :] = relaxed[q]
            middle_moved[0, rows, :] = rolled(relaxed[5], 1)
            middle_moved[1, rows, :] = rolled(relaxed[6], -1)
        inside = [q for q in range(19) if 0 <= layer - LINKS[q][0] <= 2]
        if layer == 1:
            copies.append(pltpu.make_async_copy(buffer.at[:, 1], flow.at[:, 1], sems.at[0]))
            copies[-1].start()
        else:
            for q in inside:
                copies.append(
                    pltpu.make_async_copy(
                        buffer.at[q, layer], flow.at[q, layer], sems.at[1 + (layer // 2) * 19 + q]
                    )
                )
                copies[-1].start()
    for side, ref, row, link, sign in (
        (0, low, PAD - 1, 3, 1.0),
        (1, high, PAD + width, 4, -1.0),
    ):
        w = W7[link]
        for layer in range(3):
            kind, mineral, total, own = (
                ref[3 * k + layer : 3 * k + layer + 1, :] for k in range(19, 23)
            )
            rate = jnp.full((1, LX), rates[0], jnp.float32)
            goal = jnp.full((1, LX), target[0], jnp.float32)
            for k in range(1, rates.shape[0]):
                rate = jnp.where(mineral == float(k), rates[k], rate)
                goal = jnp.where(mineral == float(k), target[k], goal)
            reaction = jnp.where(kind == 2.0, -rate * (total - goal), 0.0)
            base = KEEP_S * own + (w * GAIN_S) * total + w * reaction
            slope = (sign * 4.0 * w * GAIN_S) * total
            density, _, my, _ = sums(pull(layer, row, 1, zero1))
            if layer == 1:
                middle[link, row : row + 1, :] = base + slope * (my / density)
            else:
                at = 2 * side + layer // 2
                edge_part[0, at : at + 1, :] = density
                edge_part[1, at : at + 1, :] = my
                edge_chem[0, at : at + 1, :] = base
                edge_chem[1, at : at + 1, :] = slope
    for copy in copies:
        copy.wait()


def relax_solute(s, total, reaction, inverse, momenta):
    common = (W7[1] * GAIN_S) * total + W7[1] * reaction
    slope = (4.0 * W7[1] * GAIN_S) * total * inverse
    out = [KEEP_S * s[0] + (W7[0] * GAIN_S) * total + W7[0] * reaction]
    for q, m in zip((1, 3, 5), momenta):
        out.append(KEEP_S * s[q] + common + slope * m)
        out.append(KEEP_S * s[q + 1] + common - slope * m)
    return out


def outer_kernel(
    pop,
    sol,
    pore,
    chem,
    moved,
    kept,
    mask,
    part,
    edge_part,
    edge_chem,
    middle,
    middle_moved,
    across,
    on_chip,
    flow_in,
    flow,
    solute,
    faces,
    faces_moved,
    cross_s,
    fbuf,
    sbuf,
    sems,
):
    del flow_in
    width = pop.shape[2]
    tiles = width // 8
    span = width + SPAN
    own = readers(moved, kept, mask)

    def body(above, below):
        def value(q, layer, row, count):
            ref, links = (below, UP) if layer == -1 else (above, DOWN)
            at = links.index(q) * span + row - PAD + 2
            return ref[at : at + count, :]

        def shifted(q, layer, row, count):
            if 0 <= layer <= 2:
                return own[0](q, layer, row, count)
            return rolled(value(q, layer, row, count), LINKS[q][2])

        def plain(q, layer, row, count):
            if 0 <= layer <= 2:
                return own[1](q, layer, row, count)
            return value(q, layer, row, count)

        def masks(ex, layer, row, count):
            if 0 <= layer <= 2:
                return own[2](ex, layer, row, count)
            at = 5 * span + row - PAD + 2
            return rolled((below if layer == -1 else above)[at : at + count, :], ex)

        copies = []

        def send(src, dst):
            copies.append(pltpu.make_async_copy(src, dst, sems.at[len(copies)]))
            copies[-1].start()

        for side, ref, layer, outside, enter, leave in (
            (0, below, 0, -1, UP, DOWN),
            (1, above, 2, 3, DOWN, UP),
        ):
            sign = 1.0 if side == 0 else -1.0
            for t in range(tiles):
                row, rows = PAD + 8 * t, slice(8 * t, 8 * t + 8)
                rock = pore[layer, rows, :] == 0
                f = {q: streamed(q, layer, row, 8, shifted, plain, masks) for q in enter}
                for k, q in enumerate(enter):
                    fbuf[side, k, rows, :] = jnp.where(rock, pop[q, layer, rows, :], f[q])
                density, mz, my, mx = (part[side, k, rows, :] for k in range(4))
                arrived = add_all(f.values())
                density = density + arrived
                mz = mz + sign * arrived
                for q in enter:
                    _, ey, ex = LINKS[q]
                    if ey:
                        my = my + f[q] if ey == 1 else my - f[q]
                    if ex:
                        mx = mx + f[q] if ex == 1 else mx - f[q]
                relaxed = relax_solute(
                    [sol[q, layer, rows, :] for q in range(7)],
                    chem[0, layer, rows, :],
                    chem[1, layer, rows, :],
                    jnp.where(rock, 0.0, 1.0 / density),
                    (mz, my, mx),
                )
                into = slice(row, row + 8)
                for q in range(7):
                    faces[q, side, into, :] = relaxed[q]
                faces_moved[0, side, rows, :] = rolled(relaxed[5], 1)
                faces_moved[1, side, rows, :] = rolled(relaxed[6], -1)
                back = add_all(
                    streamed(q, outside, row, 8, shifted, plain, masks) for q in leave
                )
                base, partial, weight = (
                    ref[6 * span + k * width + 8 * t : 6 * span + k * width + 8 * t + 8, :]
                    for k in range(3)
                )
                cross_s[side, rows, :] = base + weight / (partial + back)
            for k, q in enumerate(enter):
                send(fbuf.at[side, k], flow.at[q, layer])
            for end, row, link in ((0, PAD - 1, 3), (1, PAD + width, 4)):
                at = 2 * end + side
                line = slice(at, at + 1)
                f = {q: streamed(q, layer, row, 1, shifted, plain, masks) for q in enter}
                density = edge_part[0, line, :] + add_all(f.values())
                my = edge_part[1, line, :]
                for q in enter:
                    if LINKS[q][1]:
                        my = my + f[q] if LINKS[q][1] == 1 else my - f[q]
                faces[link, side, row : row + 1, :] = edge_chem[0, line, :] + edge_chem[
                    1, line, :
                ] * (my / density)

        def solute_at(q, layer, row, count):
            if layer == 1:
                return middle[q, row : row + count, :]
            return faces[q, layer // 2, row : row + count, :]

        for layer in (1, 0, 2):
            for t in range(tiles):
                row, rows = PAD + 8 * t, slice(8 * t, 8 * t + 8)
                rock = pore[layer, rows, :] == 0
                for q in range(7):
                    ez, ey, ex = LINKS[q]
                    src = layer - ez
                    if src == -1:
                        v = cross_s[0, rows, :]
                    elif src == 3:
                        v = cross_s[1, rows, :]
                    elif ex and layer == 1:
                        v = middle_moved[q - 5, rows, :]
                    elif ex:
                        v = faces_moved[q - 5, layer // 2, rows, :]
                    else:
                        v = solute_at(q, src, row - ey, 8)
                    if q:
                        open_ = masks(ex, src, row - ey, 8) > 0.0
                        v = jnp.where(open_, v, solute_at(REVERSE[q], layer, row, 8))
                    sbuf[q, layer, rows, :] = jnp.where(rock, sol[q, layer, rows, :], v)
            send(sbuf.at[:, layer], solute.at[:, layer])
        for copy in copies:
            copy.wait()

    by_parity(body, on_chip, across)


VMEM = pl.BlockSpec(memory_space=pltpu.VMEM)
SMEM = pl.BlockSpec(memory_space=pltpu.SMEM)
ANY = pl.BlockSpec(memory_space=pl.ANY)
HBM = pl.BlockSpec(memory_space=pltpu.HBM)
DMA = pltpu.SemaphoreType.DMA


def call(kernel, operands, specs, outs, scratch=(), aliases=None, flops=1_000_000):
    return pl.pallas_call(
        kernel,
        out_shape=[jax.ShapeDtypeStruct(s, jnp.float32) for s, _ in outs],
        in_specs=list(specs),
        out_specs=[spec for _, spec in outs],
        scratch_shapes=[pltpu.VMEM(s, jnp.float32) if isinstance(s, tuple) else s for s in scratch],
        input_output_aliases=aliases or {},
        compiler_params=pltpu.CompilerParams(vmem_limit_bytes=MAX_VMEM),
        cost_estimate=pl.CostEstimate(flops=flops, bytes_accessed=1_000_000, transcendentals=0),
        name=kernel.__name__,
    )(*operands)


def on_device(populations, solute, pore_mask, mineral_ids, reaction_rates, saturation):
    width = pore_mask.shape[1]
    padded = width + 2 * PAD
    cells = (populations, solute, pore_mask, mineral_ids)
    tables = (reaction_rates, saturation)
    gz, gy = lax.axis_size("gz"), lax.axis_size("gy")
    edges = call(
        pack_edges,
        tuple(pltpu.with_memory_space_constraint(v, pltpu.HBM) for v in cells),
        [HBM] * 4,
        [((EDGE_ROWS, LX), VMEM)] * 2,
        [
            (2, 19, 3, 8, LX),
            (2, 7, 3, 8, LX),
            pltpu.VMEM((2, 3, 8, LX), jnp.int32),
            pltpu.VMEM((2, 3, 8, LX), jnp.int32),
            (2, 3, NEAR, 8, LX),
            DMA((2, 4)),
        ],
    )
    low = lax.ppermute(edges[0], "gy", [(i, i + 1) for i in range(gy - 1)])
    high = lax.ppermute(edges[1], "gy", [(i + 1, i) for i in range(gy - 1)])
    whole = ((19, 3, padded, LX), VMEM)
    masks = ((3, 3, padded, LX), VMEM)
    moved, kept, mask, chem = call(
        relax_kernel,
        cells + tables,
        [VMEM] * 4 + [SMEM] * 2,
        [whole, whole, masks, ((2, 3, width, LX), VMEM)],
        flops=6_000_000,
    )
    rows = 9 * width + 6 * SPAN
    moved, kept, mask, across, on_chip = call(
        face_kernel,
        (moved, kept, mask, low, high, solute, chem),
        [VMEM] * 7,
        [whole, whole, masks, ((rows, LX), VMEM), ((rows, LX), VMEM)],
        [(2, 2, EDGE_ROWS, LX)],
        {0: 0, 1: 1, 2: 2},
    )
    across = lax.ppermute(
        across, "gz", [(i, (i + 1 if i % 2 else i - 1) % gz) for i in range(gz)]
    )
    on_chip = lax.ppermute(on_chip, "gz", [(i, i + 1 - 2 * (i % 2)) for i in range(gz)])
    flow, part, edge_part, edge_chem, middle, middle_moved = call(
        inner_kernel,
        cells[:3] + (chem, moved, kept, mask, low, high) + tables,
        [VMEM] * 9 + [SMEM] * 2,
        [
            (populations.shape, ANY),
            ((2, 4, width, LX), VMEM),
            ((2, 8, LX), VMEM),
            ((2, 8, LX), VMEM),
            ((7, padded, LX), VMEM),
            ((2, width, LX), VMEM),
        ],
        [(19, 3, width, LX), DMA((39,))],
        flops=6_000_000,
    )
    return tuple(
        call(
            outer_kernel,
            cells[:3]
            + (chem, moved, kept, mask, part, edge_part, edge_chem, middle, middle_moved)
            + (across, on_chip, flow),
            [VMEM] * 14 + [ANY],
            [(populations.shape, ANY), (solute.shape, ANY)],
            [
                (7, 2, padded, LX),
                (2, 2, width, LX),
                (2, width, LX),
                (2, 5, width, LX),
                (7, 3, width, LX),
                DMA((13,)),
            ],
            {14: 0},
        )
    )


def solution(mesh):
    cells = P(None, "gz", "gy", None)
    return jax.shard_map(
        on_device,
        mesh=mesh,
        in_specs=(cells, cells, P("gz", "gy", None), P("gz", "gy", None), P(), P()),
        out_specs=(cells, cells),
        check_vma=False,
    )
```

```python
import functools

import jax
import jax.numpy as jnp
import numpy as np
from jax import lax
from jax.experimental import pallas as pl
from jax.experimental.pallas import tpu as pltpu
from jax.sharding import PartitionSpec as P

LINKS = (
    (0, 0, 0),
    (1, 0, 0),
    (-1, 0, 0),
    (0, 1, 0),
    (0, -1, 0),
    (0, 0, 1),
    (0, 0, -1),
    (1, 1, 0),
    (-1, -1, 0),
    (1, -1, 0),
    (-1, 1, 0),
    (1, 0, 1),
    (-1, 0, -1),
    (1, 0, -1),
    (-1, 0, 1),
    (0, 1, 1),
    (0, -1, -1),
    (0, 1, -1),
    (0, -1, 1),
)
REVERSE = (0, 2, 1, 4, 3, 6, 5, 8, 7, 10, 9, 12, 11, 14, 13, 16, 15, 18, 17)
W19 = (1.0 / 3.0,) + (1.0 / 18.0,) * 6 + (1.0 / 36.0,) * 12
W7 = (0.25,) + (0.125,) * 6
UP = tuple(q for q in range(19) if LINKS[q][0] == 1)
DOWN = tuple(q for q in range(19) if LINKS[q][0] == -1)
KEEP = 1.0 - 1.0 / 1.25
GAIN = 1.0 / 1.25
KEEP_S = 1.0 - 1.0 / 1.4
GAIN_S = 1.0 / 1.4
LX = 128
PAD = 8
MAX_VMEM = 12 * 1024 * 1024
NEAR = 23
FAR_ROWS = 3 * NEAR
EDGE_ROWS = 88
SPAN = 4


def relax(p):
    d = {q: p[q] - p[q + 1] for q in range(1, 19, 2)}
    s = {q: p[q] + p[q + 1] for q in range(1, 19, 2)}
    density = p[0] + (
        ((s[1] + s[3]) + (s[5] + s[7])) + ((s[9] + s[11]) + (s[13] + s[15])) + s[17]
    )
    mz = (d[1] + d[7]) + (d[9] + d[11]) + d[13]
    my = (d[3] + d[7]) + (d[15] + d[17]) - d[9]
    mx = (d[5] + d[11]) + (d[15] - d[13]) - d[17]
    inverse = 1.0 / density
    uz, uy, ux = mz * inverse, my * inverse, mx * inverse
    rest = 1.0 - 1.5 * (uz * uz + uy * uy + ux * ux)
    out = [None] * 19
    scaled = {w: density * (GAIN * w) for w in set(W19)}
    out[0] = KEEP * p[0] + scaled[W19[0]] * rest
    along = {
        1: uz,
        3: uy,
        5: ux,
        7: uz + uy,
        9: uz - uy,
        11: uz + ux,
        13: uz - ux,
        15: uy + ux,
        17: uy - ux,
    }
    for q, e in along.items():
        w = scaled[W19[q]]
        even = w * (rest + 4.5 * (e * e))
        odd = w * (3.0 * e)
        out[q] = KEEP * p[q] + (even + odd)
        out[q + 1] = KEEP * p[q + 1] + (even - odd)
    return out


def solute_terms(s, pore, ids, rates_ref, target_ref):
    total = ((s[0] + s[1]) + (s[2] + s[3])) + ((s[4] + s[5]) + s[6])
    rate = jnp.full(total.shape, rates_ref[0], jnp.float32)
    target = jnp.full(total.shape, target_ref[0], jnp.float32)
    for k in range(1, rates_ref.shape[0]):
        rate = jnp.where(ids == k, rates_ref[k], rate)
        target = jnp.where(ids == k, target_ref[k], target)
    reaction = jnp.where(pore == 2, -rate * (total - target), 0.0)
    return total, reaction


def rolled(value, shift):
    return value if shift == 0 else pltpu.roll(value, shift % LX, axis=1)


def sums(f):
    d = {q: f[q] - f[q + 1] for q in range(1, 19, 2)}
    s = {q: f[q] + f[q + 1] for q in range(1, 19, 2)}
    density = f[0] + (
        ((s[1] + s[3]) + (s[5] + s[7])) + ((s[9] + s[11]) + (s[13] + s[15])) + s[17]
    )
    mz = (d[1] + d[7]) + (d[9] + d[11]) + d[13]
    my = (d[3] + d[7]) + (d[15] + d[17]) - d[9]
    mx = (d[5] + d[11]) + (d[15] - d[13]) - d[17]
    return density, mz, my, mx


def add_all(values):
    values = list(values)
    while len(values) > 1:
        values = [
            values[i] + values[i + 1] if i + 1 < len(values) else values[i]
            for i in range(0, len(values), 2)
        ]
    return values[0]


def toward(sign):
    return tuple(q for q in range(19) if LINKS[q][1] == sign)


def either(condition, when_true, when_false):
    pl.when(condition)(when_true)
    pl.when(jnp.logical_not(condition))(when_false)


def upper_half():
    return lax.axis_index("gz") >= lax.axis_size("gz") // 2


def by_parity(body, first, second):
    even = lax.rem(lax.axis_index("gz"), 2) == 0
    either(even, lambda: body(first, second), lambda: body(second, first))


def pack_edges(pop, sol, pore, ids, first, second, epop, esol, epore, eids, erel, sems):
    width = pop.shape[2]
    copies = []
    for side, start in ((0, width - 8), (1, 0)):
        rows = pl.ds(start, 8)
        for k, (src, dst) in enumerate(
            (
                (pop.at[:, :, rows, :], epop),
                (sol.at[:, :, rows, :], esol),
                (pore.at[:, rows, :], epore),
                (ids.at[:, rows, :], eids),
            )
        ):
            copy = pltpu.make_async_copy(src, dst.at[side], sems.at[side, k])
            copy.start()
            copies.append(copy)
    for copy in copies:
        copy.wait()
    for side, link in ((0, 3), (1, 4)):
        for layer in range(3):
            rel = relax([epop[side, q, layer] for q in range(19)])
            for q in range(19):
                erel[side, layer, q] = rel[q]
            kind = epore[side, layer].astype(jnp.float32)
            erel[side, layer, 19] = kind
            erel[side, layer, 20] = eids[side, layer].astype(jnp.float32)
            erel[side, layer, 21] = add_all(esol[side, q, layer] for q in range(7))
            erel[side, layer, 22] = esol[side, link, layer]

    def emit(up, down):
        for side, out, near, far, sign in ((0, up, 7, 6, 1), (1, down, 0, 1, -1)):
            for layer in range(3):
                for k in range(NEAR):
                    at = 3 * k + layer
                    out[at : at + 1, :] = erel[side, layer, k, near : near + 1, :]
                for k, q in enumerate(toward(sign) + (19,)):
                    at = FAR_ROWS + 3 * k + layer
                    out[at : at + 1, :] = erel[side, layer, q, far : far + 1, :]
            out[EDGE_ROWS - 1 : EDGE_ROWS, :] = jnp.zeros((1, LX), jnp.float32)

    either(upper_half(), lambda: emit(second, first), lambda: emit(first, second))


def relax_kernel(pop, sol, pore, ids, rates, target, moved, kept, mask, chem, table):
    width = pop.shape[2]
    for k in range(rates.shape[0]):
        for at, ref in ((k, rates), (k + rates.shape[0], target)):
            table[at : at + 1, :] = jnp.full((1, LX), ref[k], jnp.float32)
    for layer in range(3):
        for t in range(width // 8):
            rows, into = slice(8 * t, 8 * t + 8), slice(PAD + 8 * t, PAD + 8 * t + 8)
            out = relax([pop[q, layer, rows, :] for q in range(19)])
            for q in range(19):
                ex = LINKS[q][2]
                moved[q, layer, into, :] = rolled(out[q], ex)
                if ex:
                    kept[q, layer, into, :] = out[q]
            kind = pore[layer, rows, :]
            m = jnp.where(kind > 0, 1.0, 0.0)
            for ex in (0, 1, -1):
                mask[ex % 3, layer, into, :] = rolled(m, ex)
            s = [sol[q, layer, rows, :] for q in range(7)]
            total, reaction = solute_terms(s, kind, ids[layer, rows, :], rates, target)
            chem[0, layer, rows, :] = total
            chem[1, layer, rows, :] = reaction


def streamed(q, layer, row, count, shifted, plain, masks):
    ez, ey, ex = LINKS[q]
    value = shifted(q, layer - ez, row - ey, count)
    if q == 0:
        return value
    open_ = masks(ex, layer - ez, row - ey, count) > 0.0
    return jnp.where(open_, value, plain(REVERSE[q], layer, row, count))


def readers(moved, kept, mask):
    def shifted(q, layer, row, count):
        return moved[q, layer, row : row + count, :]

    def plain(q, layer, row, count):
        return (kept if LINKS[q][2] else moved)[q, layer, row : row + count, :]

    def masks(ex, layer, row, count):
        return mask[ex % 3, layer, row : row + count, :]

    return shifted, plain, masks


def face_kernel(
    moved_in,
    kept_in,
    mask_in,
    first,
    second,
    sol,
    chem,
    moved,
    kept,
    mask,
    across,
    on_chip,
    edges,
    turned,
):
    del moved_in, kept_in, mask_in
    width = sol.shape[2]
    upper = upper_half()
    for t in range(EDGE_ROWS // 8):
        rows = slice(8 * t, 8 * t + 8)
        for side, v in (
            (0, jnp.where(upper, second[rows, :], first[rows, :])),
            (1, jnp.where(upper, first[rows, :], second[rows, :])),
        ):
            edges[side, rows, :] = v
            turned[side, 0, rows, :] = rolled(v, 1)
            turned[side, 1, rows, :] = rolled(v, -1)
    for side, near, far, sign in (
        (0, PAD - 1, PAD - 2, 1),
        (1, PAD + width, PAD + width + 1, -1),
    ):

        def line(at, ex):
            if ex == 0:
                return edges[side, at : at + 1, :]
            return turned[side, 0 if ex == 1 else 1, at : at + 1, :]

        for layer in range(3):
            for row, start, links in (
                (near, 0, tuple(range(19))),
                (far, FAR_ROWS, toward(sign)),
            ):
                into = slice(row, row + 1)
                for k, q in enumerate(links):
                    at, ex = start + 3 * k + layer, LINKS[q][2]
                    moved[q, layer, into, :] = line(at, ex)
                    if ex:
                        kept[q, layer, into, :] = line(at, 0)
                at = start + 3 * len(links) + layer
                for ex in (0, 1, -1):
                    mask[ex % 3, layer, into, :] = line(at, ex)
    shifted, plain, masks = readers(moved, kept, mask)

    def emit(up, down):
        span = width + SPAN
        for out, layer, cross, link in ((up, 2, UP, 1), (down, 0, DOWN, 2)):
            w = W7[link]
            for t in range(width // 8):
                row, rows = PAD + 8 * t, slice(8 * t, 8 * t + 8)
                get = functools.partial(
                    streamed,
                    layer=layer,
                    row=row,
                    count=8,
                    shifted=shifted,
                    plain=plain,
                    masks=masks,
                )
                away = add_all(get(q) for q in cross)
                level = add_all(get(q) for q in range(19) if LINKS[q][0] == 0)
                partial = level + away
                total, reaction = chem[0, layer, rows, :], chem[1, layer, rows, :]
                slope = (4.0 * w * GAIN_S) * total
                base = KEEP_S * sol[link, layer, rows, :] + (w * GAIN_S) * total + w * reaction
                for k, v in enumerate((base - slope, partial, slope * (partial + away))):
                    at = 6 * span + k * width + 8 * t
                    out[at : at + 8, :] = v
            for k in range(6):
                at = k * span
                pieces = [(PAD - 2, 2, 0)]
                pieces += [(PAD + 8 * t, 8, 2 + 8 * t) for t in range(width // 8)]
                pieces += [(PAD + width, 2, 2 + width)]
                for row, count, to in pieces:
                    v = plain(cross[k], layer, row, count) if k < 5 else masks(0, layer, row, count)
                    out[at + to : at + to + count, :] = v

    by_parity(emit, on_chip, across)


def inner_kernel(
    pop,
    sol,
    pore,
    chem,
    moved,
    kept,
    mask,
    edges,
    table,
    flow,
    part,
    edge_part,
    edge_chem,
    middle,
    middle_moved,
):
    width = pop.shape[2]
    tiles = width // 8
    shifted, plain, masks = readers(moved, kept, mask)
    zero8 = jnp.zeros((8, LX), jnp.float32)
    zero1 = jnp.zeros((1, LX), jnp.float32)

    def pull(layer, row, count, zero):
        return [
            streamed(q, layer, row, count, shifted, plain, masks)
            if 0 <= layer - LINKS[q][0] <= 2
            else zero
            for q in range(19)
        ]

    for layer in (1, 0, 2):
        for t in range(tiles):
            row, rows = PAD + 8 * t, slice(8 * t, 8 * t + 8)
            f = pull(layer, row, 8, zero8)
            rock = pore[layer, rows, :] == 0
            for q in range(19):
                if 0 <= layer - LINKS[q][0] <= 2:
                    flow[q, layer, rows, :] = jnp.where(rock, pop[q, layer, rows, :], f[q])
            density, mz, my, mx = sums(f)
            if layer != 1:
                for k, v in enumerate((density, mz, my, mx)):
                    part[layer // 2, k, rows, :] = v
                continue
            relaxed = relax_solute(
                [sol[q, layer, rows, :] for q in range(7)],
                chem[0, layer, rows, :],
                chem[1, layer, rows, :],
                jnp.where(rock, 0.0, 1.0 / density),
                (mz, my, mx),
            )
            into = slice(row, row + 8)
            for q in range(7):
                middle[q, into, :] = relaxed[q]
            middle_moved[0, rows, :] = rolled(relaxed[5], 1)
            middle_moved[1, rows, :] = rolled(relaxed[6], -1)
    for side, row, link, sign in ((0, PAD - 1, 3, 1.0), (1, PAD + width, 4, -1.0)):
        w = W7[link]
        for layer in range(3):
            kind, mineral, total, own = (
                edges[side, 3 * k + layer : 3 * k + layer + 1, :] for k in range(19, 23)
            )
            kinds = table.shape[0] // 2
            rate, goal = table[0:1, :], table[kinds : kinds + 1, :]
            for k in range(1, kinds):
                rate = jnp.where(mineral == float(k), table[k : k + 1, :], rate)
                goal = jnp.where(mineral == float(k), table[kinds + k : kinds + k + 1, :], goal)
            reaction = jnp.where(kind == 2.0, -rate * (total - goal), 0.0)
            base = KEEP_S * own + (w * GAIN_S) * total + w * reaction
            slope = (sign * 4.0 * w * GAIN_S) * total
            density, _, my, _ = sums(pull(layer, row, 1, zero1))
            if layer == 1:
                middle[link, row : row + 1, :] = base + slope * (my / density)
            else:
                at = 2 * side + layer // 2
                edge_part[0, at : at + 1, :] = density
                edge_part[1, at : at + 1, :] = my
                edge_chem[0, at : at + 1, :] = base
                edge_chem[1, at : at + 1, :] = slope


def relax_solute(s, total, reaction, inverse, momenta):
    common = (W7[1] * GAIN_S) * total + W7[1] * reaction
    slope = (4.0 * W7[1] * GAIN_S) * total * inverse
    out = [KEEP_S * s[0] + (W7[0] * GAIN_S) * total + W7[0] * reaction]
    for q, m in zip((1, 3, 5), momenta):
        out.append(KEEP_S * s[q] + common + slope * m)
        out.append(KEEP_S * s[q + 1] + common - slope * m)
    return out


def outer_kernel(
    pop,
    sol,
    pore,
    chem,
    moved,
    kept,
    mask,
    part,
    edge_part,
    edge_chem,
    middle,
    middle_moved,
    across,
    on_chip,
    inner_flow,
    flow,
    solute,
    faces,
    faces_moved,
    cross_s,
    fbuf,
    sbuf,
    sems,
):
    width = pop.shape[2]
    tiles = width // 8
    span = width + SPAN
    own = readers(moved, kept, mask)
    early = []
    for layer in (1, 0, 2):
        local = [q for q in range(19) if 0 <= layer - LINKS[q][0] <= 2]
        start = 0
        while start < len(local):
            stop = start
            while stop + 1 < len(local) and local[stop + 1] == local[stop] + 1:
                stop += 1
            links = pl.ds(local[start], local[stop] - local[start] + 1)
            copy = pltpu.make_async_copy(
                inner_flow.at[links, layer], flow.at[links, layer], sems.at[len(early)]
            )
            copy.start()
            early.append(copy)
            start = stop + 1

    def body(above, below):
        def value(q, layer, row, count):
            ref, links = (below, UP) if layer == -1 else (above, DOWN)
            at = links.index(q) * span + row - PAD + 2
            return ref[at : at + count, :]

        def shifted(q, layer, row, count):
            if 0 <= layer <= 2:
                return own[0](q, layer, row, count)
            return rolled(value(q, layer, row, count), LINKS[q][2])

        def plain(q, layer, row, count):
            if 0 <= layer <= 2:
                return own[1](q, layer, row, count)
            return value(q, layer, row, count)

        def masks(ex, layer, row, count):
            if 0 <= layer <= 2:
                return own[2](ex, layer, row, count)
            at = 5 * span + row - PAD + 2
            return rolled((below if layer == -1 else above)[at : at + count, :], ex)

        copies = []

        def send(src, dst):
            copies.append(pltpu.make_async_copy(src, dst, sems.at[len(early) + len(copies)]))
            copies[-1].start()

        for side, ref, layer, outside, enter, leave in (
            (0, below, 0, -1, UP, DOWN),
            (1, above, 2, 3, DOWN, UP),
        ):
            sign = 1.0 if side == 0 else -1.0
            for t in range(tiles):
                row, rows = PAD + 8 * t, slice(8 * t, 8 * t + 8)
                rock = pore[layer, rows, :] == 0
                f = {q: streamed(q, layer, row, 8, shifted, plain, masks) for q in enter}
                for k, q in enumerate(enter):
                    fbuf[side, k, rows, :] = jnp.where(rock, pop[q, layer, rows, :], f[q])
                density, mz, my, mx = (part[side, k, rows, :] for k in range(4))
                arrived = add_all(f.values())
                density = density + arrived
                mz = mz + sign * arrived
                for q in enter:
                    _, ey, ex = LINKS[q]
                    if ey:
                        my = my + f[q] if ey == 1 else my - f[q]
                    if ex:
                        mx = mx + f[q] if ex == 1 else mx - f[q]
                relaxed = relax_solute(
                    [sol[q, layer, rows, :] for q in range(7)],
                    chem[0, layer, rows, :],
                    chem[1, layer, rows, :],
                    jnp.where(rock, 0.0, 1.0 / density),
                    (mz, my, mx),
                )
                into = slice(row, row + 8)
                for q in range(7):
                    faces[q, side, into, :] = relaxed[q]
                faces_moved[0, side, rows, :] = rolled(relaxed[5], 1)
                faces_moved[1, side, rows, :] = rolled(relaxed[6], -1)
                back = add_all(
                    streamed(q, outside, row, 8, shifted, plain, masks) for q in leave
                )
                base, partial, weight = (
                    ref[6 * span + k * width + 8 * t : 6 * span + k * width + 8 * t + 8, :]
                    for k in range(3)
                )
                cross_s[side, rows, :] = base + weight / (partial + back)
            for k, q in enumerate(enter):
                send(fbuf.at[side, k], flow.at[q, layer])
            for end, row, link in ((0, PAD - 1, 3), (1, PAD + width, 4)):
                at = 2 * end + side
                line = slice(at, at + 1)
                f = {q: streamed(q, layer, row, 1, shifted, plain, masks) for q in enter}
                density = edge_part[0, line, :] + add_all(f.values())
                my = edge_part[1, line, :]
                for q in enter:
                    if LINKS[q][1]:
                        my = my + f[q] if LINKS[q][1] == 1 else my - f[q]
                faces[link, side, row : row + 1, :] = edge_chem[0, line, :] + edge_chem[
                    1, line, :
                ] * (my / density)

        def solute_at(q, layer, row, count):
            if layer == 1:
                return middle[q, row : row + count, :]
            return faces[q, layer // 2, row : row + count, :]

        for layer in (1, 0, 2):
            for t in range(tiles):
                row, rows = PAD + 8 * t, slice(8 * t, 8 * t + 8)
                rock = pore[layer, rows, :] == 0
                for q in range(7):
                    ez, ey, ex = LINKS[q]
                    src = layer - ez
                    if src == -1:
                        v = cross_s[0, rows, :]
                    elif src == 3:
                        v = cross_s[1, rows, :]
                    elif ex and layer == 1:
                        v = middle_moved[q - 5, rows, :]
                    elif ex:
                        v = faces_moved[q - 5, layer // 2, rows, :]
                    else:
                        v = solute_at(q, src, row - ey, 8)
                    if q:
                        open_ = masks(ex, src, row - ey, 8) > 0.0
                        v = jnp.where(open_, v, solute_at(REVERSE[q], layer, row, 8))
                    sbuf[q, layer, rows, :] = jnp.where(rock, sol[q, layer, rows, :], v)
            send(sbuf.at[:, layer], solute.at[:, layer])
        for copy in copies:
            copy.wait()

    by_parity(body, on_chip, across)
    for copy in early:
        copy.wait()


VMEM = pl.BlockSpec(memory_space=pltpu.VMEM)
SMEM = pl.BlockSpec(memory_space=pltpu.SMEM)
ANY = pl.BlockSpec(memory_space=pl.ANY)
HBM = pl.BlockSpec(memory_space=pltpu.HBM)
DMA = pltpu.SemaphoreType.DMA


def call(kernel, operands, specs, outs, scratch=(), aliases=None, flops=1_000_000):
    return pl.pallas_call(
        kernel,
        out_shape=[jax.ShapeDtypeStruct(s, jnp.float32) for s, _ in outs],
        in_specs=list(specs),
        out_specs=[spec for _, spec in outs],
        scratch_shapes=[pltpu.VMEM(s, jnp.float32) if isinstance(s, tuple) else s for s in scratch],
        input_output_aliases=aliases or {},
        compiler_params=pltpu.CompilerParams(vmem_limit_bytes=MAX_VMEM),
        cost_estimate=pl.CostEstimate(flops=flops, bytes_accessed=1_000_000, transcendentals=0),
        name=kernel.__name__,
    )(*operands)


def on_device(populations, solute, pore_mask, mineral_ids, reaction_rates, saturation):
    width = pore_mask.shape[1]
    padded = width + 2 * PAD
    cells = (populations, solute, pore_mask, mineral_ids)
    tables = (reaction_rates, saturation)
    gz, gy = lax.axis_size("gz"), lax.axis_size("gy")
    first, second = call(
        pack_edges,
        tuple(pltpu.with_memory_space_constraint(v, pltpu.HBM) for v in cells),
        [HBM] * 4,
        [((EDGE_ROWS, LX), VMEM)] * 2,
        [
            (2, 19, 3, 8, LX),
            (2, 7, 3, 8, LX),
            pltpu.VMEM((2, 3, 8, LX), jnp.int32),
            pltpu.VMEM((2, 3, 8, LX), jnp.int32),
            (2, 3, NEAR, 8, LX),
            DMA((2, 4)),
        ],
    )
    def pairs(upward):
        found = []
        for place in range(gz * gy):
            ends = (place, place + 1)
            if ends[1] % gy:
                found.append(ends if upward == (place < gz // 2 * gy) else ends[::-1])
        return found

    first = lax.ppermute(first, ("gz", "gy"), pairs(True))
    second = lax.ppermute(second, ("gz", "gy"), pairs(False))
    whole = ((19, 3, padded, LX), VMEM)
    masks = ((3, 3, padded, LX), VMEM)
    moved, kept, mask, chem, table = call(
        relax_kernel,
        cells + tables,
        [VMEM] * 4 + [SMEM] * 2,
        [
            whole,
            whole,
            masks,
            ((2, 3, width, LX), VMEM),
            ((2 * reaction_rates.shape[0], LX), VMEM),
        ],
        flops=6_000_000,
    )
    rows = 9 * width + 6 * SPAN
    moved, kept, mask, across, on_chip, edges = call(
        face_kernel,
        (moved, kept, mask, first, second, solute, chem),
        [VMEM] * 7,
        [
            whole,
            whole,
            masks,
            ((rows, LX), VMEM),
            ((rows, LX), VMEM),
            ((2, EDGE_ROWS, LX), VMEM),
        ],
        [(2, 2, EDGE_ROWS, LX)],
        {0: 0, 1: 1, 2: 2},
    )
    across = lax.ppermute(
        across, "gz", [(i, (i + 1 if i % 2 else i - 1) % gz) for i in range(gz)]
    )
    on_chip = lax.ppermute(on_chip, "gz", [(i, i + 1 - 2 * (i % 2)) for i in range(gz)])
    flow, part, edge_part, edge_chem, middle, middle_moved = call(
        inner_kernel,
        (populations, solute, pore_mask, chem, moved, kept, mask, edges, table),
        [VMEM] * 9,
        [
            (populations.shape, VMEM),
            ((2, 4, width, LX), VMEM),
            ((2, 8, LX), VMEM),
            ((2, 8, LX), VMEM),
            ((7, padded, LX), VMEM),
            ((2, width, LX), VMEM),
        ],
        flops=6_000_000,
    )
    return tuple(
        call(
            outer_kernel,
            cells[:3]
            + (chem, moved, kept, mask, part, edge_part, edge_chem, middle, middle_moved)
            + (across, on_chip, flow),
            [VMEM] * 15,
            [(populations.shape, ANY), (solute.shape, ANY)],
            [
                (7, 2, padded, LX),
                (2, 2, width, LX),
                (2, width, LX),
                (2, 5, width, LX),
                (7, 3, width, LX),
                DMA((26,)),
            ],
        )
    )


def solution(mesh):
    cells = P(None, "gz", "gy", None)
    return jax.shard_map(
        on_device,
        mesh=mesh,
        in_specs=(cells, cells, P("gz", "gy", None), P("gz", "gy", None), P(), P()),
        out_specs=(cells, cells),
        check_vma=False,
    )
```

```python
import functools

import jax
import jax.numpy as jnp
import numpy as np
from jax import lax
from jax.experimental import pallas as pl
from jax.experimental.pallas import tpu as pltpu
from jax.sharding import PartitionSpec as P

LINKS = (
    (0, 0, 0),
    (1, 0, 0),
    (-1, 0, 0),
    (0, 1, 0),
    (0, -1, 0),
    (0, 0, 1),
    (0, 0, -1),
    (1, 1, 0),
    (-1, -1, 0),
    (1, -1, 0),
    (-1, 1, 0),
    (1, 0, 1),
    (-1, 0, -1),
    (1, 0, -1),
    (-1, 0, 1),
    (0, 1, 1),
    (0, -1, -1),
    (0, 1, -1),
    (0, -1, 1),
)
REVERSE = (0, 2, 1, 4, 3, 6, 5, 8, 7, 10, 9, 12, 11, 14, 13, 16, 15, 18, 17)
W19 = (1.0 / 3.0,) + (1.0 / 18.0,) * 6 + (1.0 / 36.0,) * 12
W7 = (0.25,) + (0.125,) * 6
UP = tuple(q for q in range(19) if LINKS[q][0] == 1)
DOWN = tuple(q for q in range(19) if LINKS[q][0] == -1)
KEEP = 1.0 - 1.0 / 1.25
GAIN = 1.0 / 1.25
KEEP_S = 1.0 - 1.0 / 1.4
GAIN_S = 1.0 / 1.4
LX = 128
PAD = 8
MAX_VMEM = 12 * 1024 * 1024
NEAR = 23
FAR_ROWS = 3 * NEAR
EDGE_ROWS = 88
SPAN = 4


def relax(p):
    d = {q: p[q] - p[q + 1] for q in range(1, 19, 2)}
    s = {q: p[q] + p[q + 1] for q in range(1, 19, 2)}
    density = p[0] + (
        ((s[1] + s[3]) + (s[5] + s[7])) + ((s[9] + s[11]) + (s[13] + s[15])) + s[17]
    )
    mz = (d[1] + d[7]) + (d[9] + d[11]) + d[13]
    my = (d[3] + d[7]) + (d[15] + d[17]) - d[9]
    mx = (d[5] + d[11]) + (d[15] - d[13]) - d[17]
    inverse = 1.0 / density
    uz, uy, ux = mz * inverse, my * inverse, mx * inverse
    rest = 1.0 - 1.5 * (uz * uz + uy * uy + ux * ux)
    out = [None] * 19
    scaled = {w: density * (GAIN * w) for w in set(W19)}
    out[0] = KEEP * p[0] + scaled[W19[0]] * rest
    along = {
        1: uz,
        3: uy,
        5: ux,
        7: uz + uy,
        9: uz - uy,
        11: uz + ux,
        13: uz - ux,
        15: uy + ux,
        17: uy - ux,
    }
    for q, e in along.items():
        w = scaled[W19[q]]
        even = w * (rest + 4.5 * (e * e))
        odd = w * (3.0 * e)
        out[q] = KEEP * p[q] + (even + odd)
        out[q + 1] = KEEP * p[q + 1] + (even - odd)
    return out


def pick(ids, table):
    kinds = table.shape[0] // 2
    rate, goal = table[0:1, :], table[kinds : kinds + 1, :]
    for k in range(1, kinds):
        rate = jnp.where(ids == k, table[k : k + 1, :], rate)
        goal = jnp.where(ids == k, table[kinds + k : kinds + k + 1, :], goal)
    return rate, goal


def solute_terms(s, pore, ids, table):
    total = ((s[0] + s[1]) + (s[2] + s[3])) + ((s[4] + s[5]) + s[6])
    rate, goal = pick(ids, table)
    return total, jnp.where(pore == 2, -rate * (total - goal), 0.0)


def rolled(value, shift):
    return value if shift == 0 else pltpu.roll(value, shift % LX, axis=1)


def sums(f):
    d = {q: f[q] - f[q + 1] for q in range(1, 19, 2)}
    s = {q: f[q] + f[q + 1] for q in range(1, 19, 2)}
    density = f[0] + (
        ((s[1] + s[3]) + (s[5] + s[7])) + ((s[9] + s[11]) + (s[13] + s[15])) + s[17]
    )
    mz = (d[1] + d[7]) + (d[9] + d[11]) + d[13]
    my = (d[3] + d[7]) + (d[15] + d[17]) - d[9]
    mx = (d[5] + d[11]) + (d[15] - d[13]) - d[17]
    return density, mz, my, mx


def add_all(values):
    values = list(values)
    while len(values) > 1:
        values = [
            values[i] + values[i + 1] if i + 1 < len(values) else values[i]
            for i in range(0, len(values), 2)
        ]
    return values[0]


def toward(sign):
    return tuple(q for q in range(19) if LINKS[q][1] == sign)


def either(condition, when_true, when_false):
    pl.when(condition)(when_true)
    pl.when(jnp.logical_not(condition))(when_false)


def upper_half():
    return lax.axis_index("gz") >= lax.axis_size("gz") // 2


def by_parity(body, first, second):
    even = lax.rem(lax.axis_index("gz"), 2) == 0
    either(even, lambda: body(first, second), lambda: body(second, first))


def pack_edges(
    pop,
    sol,
    pore,
    ids,
    rates,
    target,
    first,
    second,
    table,
    epop,
    esol,
    epore,
    eids,
    erel,
    srates,
    starget,
    sems,
):
    width = pop.shape[2]
    for side, start, to in ((0, width - 2, 6), (1, 0, 0)):
        rows, into = pl.ds(start, 2), pl.ds(to, 2)
        for src, dst in (
            (pop.at[:, :, rows, :], epop.at[side, :, :, into, :]),
            (sol.at[:, :, rows, :], esol.at[side, :, :, into, :]),
            (pore.at[:, rows, :], epore.at[side, :, into, :]),
            (ids.at[:, rows, :], eids.at[side, :, into, :]),
        ):
            pltpu.make_async_copy(src, dst, sems.at[0]).start()
    constants = [
        pltpu.make_async_copy(rates, srates, sems.at[1]),
        pltpu.make_async_copy(target, starget, sems.at[2]),
    ]
    for copy in constants:
        copy.start()
    every = erel.at[0, :, pl.ds(0, 14)]
    pltpu.make_async_copy(every, every, sems.at[0]).wait()
    for copy in constants:
        copy.wait()
    for side, link in ((0, 3), (1, 4)):
        for layer in range(3):
            rel = relax([epop[side, q, layer] for q in range(19)])
            for q in range(19):
                erel[side, layer, q] = rel[q]
            kind = epore[side, layer].astype(jnp.float32)
            erel[side, layer, 19] = kind
            erel[side, layer, 20] = eids[side, layer].astype(jnp.float32)
            erel[side, layer, 21] = add_all(esol[side, q, layer] for q in range(7))
            erel[side, layer, 22] = esol[side, link, layer]

    def emit(up, down):
        for side, out, near, far, sign in ((0, up, 7, 6, 1), (1, down, 0, 1, -1)):
            for layer in range(3):
                for k in range(NEAR):
                    at = 3 * k + layer
                    out[at : at + 1, :] = erel[side, layer, k, near : near + 1, :]
                for k, q in enumerate(toward(sign) + (19,)):
                    at = FAR_ROWS + 3 * k + layer
                    out[at : at + 1, :] = erel[side, layer, q, far : far + 1, :]
            out[EDGE_ROWS - 1 : EDGE_ROWS, :] = jnp.zeros((1, LX), jnp.float32)

    either(upper_half(), lambda: emit(second, first), lambda: emit(first, second))
    kinds = srates.shape[0]
    for k in range(kinds):
        for at, ref in ((k, srates), (k + kinds, starget)):
            table[at : at + 1, :] = jnp.full((1, LX), ref[k], jnp.float32)


def relax_kernel(pop, sol, pore, ids, table, moved, kept, mask, chem):
    width = pop.shape[2]
    for layer in range(3):
        for t in range(width // 8):
            rows, into = slice(8 * t, 8 * t + 8), slice(PAD + 8 * t, PAD + 8 * t + 8)
            out = relax([pop[q, layer, rows, :] for q in range(19)])
            for q in range(19):
                ex = LINKS[q][2]
                moved[q, layer, into, :] = rolled(out[q], ex)
                if ex:
                    kept[q, layer, into, :] = out[q]
            kind = pore[layer, rows, :]
            m = jnp.where(kind > 0, 1.0, 0.0)
            for ex in (0, 1, -1):
                mask[ex % 3, layer, into, :] = rolled(m, ex)
            s = [sol[q, layer, rows, :] for q in range(7)]
            total, reaction = solute_terms(s, kind, ids[layer, rows, :], table)
            chem[0, layer, rows, :] = total
            chem[1, layer, rows, :] = reaction


def streamed(q, layer, row, count, shifted, plain, masks):
    ez, ey, ex = LINKS[q]
    value = shifted(q, layer - ez, row - ey, count)
    if q == 0:
        return value
    open_ = masks(ex, layer - ez, row - ey, count) > 0.0
    return jnp.where(open_, value, plain(REVERSE[q], layer, row, count))


def readers(moved, kept, mask):
    def shifted(q, layer, row, count):
        return moved[q, layer, row : row + count, :]

    def plain(q, layer, row, count):
        return (kept if LINKS[q][2] else moved)[q, layer, row : row + count, :]

    def masks(ex, layer, row, count):
        return mask[ex % 3, layer, row : row + count, :]

    return shifted, plain, masks


def face_kernel(
    moved_in,
    kept_in,
    mask_in,
    first,
    second,
    sol,
    chem,
    moved,
    kept,
    mask,
    across,
    on_chip,
    edges,
    turned,
):
    del moved_in, kept_in, mask_in
    width = sol.shape[2]
    upper = upper_half()
    for t in range(EDGE_ROWS // 8):
        rows = slice(8 * t, 8 * t + 8)
        for side, v in (
            (0, jnp.where(upper, second[rows, :], first[rows, :])),
            (1, jnp.where(upper, first[rows, :], second[rows, :])),
        ):
            edges[side, rows, :] = v
            turned[side, 0, rows, :] = rolled(v, 1)
            turned[side, 1, rows, :] = rolled(v, -1)
    for side, near, far, sign in (
        (0, PAD - 1, PAD - 2, 1),
        (1, PAD + width, PAD + width + 1, -1),
    ):

        def line(at, ex):
            if ex == 0:
                return edges[side, at : at + 1, :]
            return turned[side, 0 if ex == 1 else 1, at : at + 1, :]

        for layer in range(3):
            for row, start, links in (
                (near, 0, tuple(range(19))),
                (far, FAR_ROWS, toward(sign)),
            ):
                into = slice(row, row + 1)
                for k, q in enumerate(links):
                    at, ex = start + 3 * k + layer, LINKS[q][2]
                    moved[q, layer, into, :] = line(at, ex)
                    if ex:
                        kept[q, layer, into, :] = line(at, 0)
                at = start + 3 * len(links) + layer
                for ex in (0, 1, -1):
                    mask[ex % 3, layer, into, :] = line(at, ex)
    shifted, plain, masks = readers(moved, kept, mask)

    def emit(up, down):
        span = width + SPAN
        for out, layer, cross, link in ((up, 2, UP, 1), (down, 0, DOWN, 2)):
            w = W7[link]
            for t in range(width // 8):
                row, rows = PAD + 8 * t, slice(8 * t, 8 * t + 8)
                get = functools.partial(
                    streamed,
                    layer=layer,
                    row=row,
                    count=8,
                    shifted=shifted,
                    plain=plain,
                    masks=masks,
                )
                away = add_all(get(q) for q in cross)
                level = add_all(get(q) for q in range(19) if LINKS[q][0] == 0)
                partial = level + away
                total, reaction = chem[0, layer, rows, :], chem[1, layer, rows, :]
                slope = (4.0 * w * GAIN_S) * total
                base = KEEP_S * sol[link, layer, rows, :] + (w * GAIN_S) * total + w * reaction
                for k, v in enumerate((base - slope, partial, slope * (partial + away))):
                    at = 6 * span + k * width + 8 * t
                    out[at : at + 8, :] = v
            for k in range(6):
                at = k * span
                pieces = [(PAD - 2, 2, 0)]
                pieces += [(PAD + 8 * t, 8, 2 + 8 * t) for t in range(width // 8)]
                pieces += [(PAD + width, 2, 2 + width)]
                for row, count, to in pieces:
                    v = plain(cross[k], layer, row, count) if k < 5 else masks(0, layer, row, count)
                    out[at + to : at + to + count, :] = v

    by_parity(emit, on_chip, across)


def inner_kernel(
    pop,
    sol,
    pore,
    chem,
    moved,
    kept,
    mask,
    edges,
    table,
    flow,
    outer_flow,
    part,
    edge_part,
    edge_chem,
    middle,
    middle_moved,
    buffer,
    sem,
):
    width = pop.shape[2]
    tiles = width // 8
    shifted, plain, masks = readers(moved, kept, mask)
    zero8 = jnp.zeros((8, LX), jnp.float32)
    zero1 = jnp.zeros((1, LX), jnp.float32)

    def pull(layer, row, count, zero):
        return [
            streamed(q, layer, row, count, shifted, plain, masks)
            if 0 <= layer - LINKS[q][0] <= 2
            else zero
            for q in range(19)
        ]

    for layer in (1, 0, 2):
        for t in range(tiles):
            row, rows = PAD + 8 * t, slice(8 * t, 8 * t + 8)
            f = pull(layer, row, 8, zero8)
            rock = pore[layer, rows, :] == 0
            for q in range(19):
                if 0 <= layer - LINKS[q][0] <= 2:
                    v = jnp.where(rock, pop[q, layer, rows, :], f[q])
                    if layer == 1:
                        buffer[q, rows, :] = v
                    else:
                        outer_flow[q, layer // 2, rows, :] = v
            density, mz, my, mx = sums(f)
            if layer != 1:
                for k, v in enumerate((density, mz, my, mx)):
                    part[layer // 2, k, rows, :] = v
                continue
            relaxed = relax_solute(
                [sol[q, layer, rows, :] for q in range(7)],
                chem[0, layer, rows, :],
                chem[1, layer, rows, :],
                jnp.where(rock, 0.0, 1.0 / density),
                (mz, my, mx),
            )
            into = slice(row, row + 8)
            for q in range(7):
                middle[q, into, :] = relaxed[q]
            middle_moved[0, rows, :] = rolled(relaxed[5], 1)
            middle_moved[1, rows, :] = rolled(relaxed[6], -1)
        if layer == 1:
            copy = pltpu.make_async_copy(buffer, flow.at[:, 1], sem)
            copy.start()
    for side, row, link, sign in ((0, PAD - 1, 3, 1.0), (1, PAD + width, 4, -1.0)):
        w = W7[link]
        for layer in range(3):
            kind, mineral, total, own = (
                edges[side, 3 * k + layer : 3 * k + layer + 1, :] for k in range(19, 23)
            )
            rate, goal = pick(mineral, table)
            reaction = jnp.where(kind == 2.0, -rate * (total - goal), 0.0)
            base = KEEP_S * own + (w * GAIN_S) * total + w * reaction
            slope = (sign * 4.0 * w * GAIN_S) * total
            density, _, my, _ = sums(pull(layer, row, 1, zero1))
            if layer == 1:
                middle[link, row : row + 1, :] = base + slope * (my / density)
            else:
                at = 2 * side + layer // 2
                edge_part[0, at : at + 1, :] = density
                edge_part[1, at : at + 1, :] = my
                edge_chem[0, at : at + 1, :] = base
                edge_chem[1, at : at + 1, :] = slope
    copy.wait()


def relax_solute(s, total, reaction, inverse, momenta):
    common = (W7[1] * GAIN_S) * total + W7[1] * reaction
    slope = (4.0 * W7[1] * GAIN_S) * total * inverse
    out = [KEEP_S * s[0] + (W7[0] * GAIN_S) * total + W7[0] * reaction]
    for q, m in zip((1, 3, 5), momenta):
        out.append(KEEP_S * s[q] + common + slope * m)
        out.append(KEEP_S * s[q + 1] + common - slope * m)
    return out


def outer_kernel(
    pop,
    sol,
    pore,
    chem,
    moved,
    kept,
    mask,
    part,
    edge_part,
    edge_chem,
    middle,
    middle_moved,
    across,
    on_chip,
    outer_flow,
    flow_in,
    flow,
    solute,
    faces,
    faces_moved,
    cross_s,
    fbuf,
    sbuf,
    sems,
):
    del flow_in
    width = pop.shape[2]
    tiles = width // 8
    span = width + SPAN
    own = readers(moved, kept, mask)
    for layer in (0, 2):
        local = [q for q in range(19) if 0 <= layer - LINKS[q][0] <= 2]
        start = 0
        while start < len(local):
            stop = start
            while stop + 1 < len(local) and local[stop + 1] == local[stop] + 1:
                stop += 1
            links = pl.ds(local[start], local[stop] - local[start] + 1)
            pltpu.make_async_copy(
                outer_flow.at[links, layer // 2], flow.at[links, layer], sems.at[0]
            ).start()
            start = stop + 1

    def body(above, below):
        def value(q, layer, row, count):
            ref, links = (below, UP) if layer == -1 else (above, DOWN)
            at = links.index(q) * span + row - PAD + 2
            return ref[at : at + count, :]

        def shifted(q, layer, row, count):
            if 0 <= layer <= 2:
                return own[0](q, layer, row, count)
            return rolled(value(q, layer, row, count), LINKS[q][2])

        def plain(q, layer, row, count):
            if 0 <= layer <= 2:
                return own[1](q, layer, row, count)
            return value(q, layer, row, count)

        def masks(ex, layer, row, count):
            if 0 <= layer <= 2:
                return own[2](ex, layer, row, count)
            at = 5 * span + row - PAD + 2
            return rolled((below if layer == -1 else above)[at : at + count, :], ex)

        for side, ref, layer, outside, enter, leave in (
            (0, below, 0, -1, UP, DOWN),
            (1, above, 2, 3, DOWN, UP),
        ):
            sign = 1.0 if side == 0 else -1.0
            for t in range(tiles):
                row, rows = PAD + 8 * t, slice(8 * t, 8 * t + 8)
                rock = pore[layer, rows, :] == 0
                f = {q: streamed(q, layer, row, 8, shifted, plain, masks) for q in enter}
                for k, q in enumerate(enter):
                    fbuf[side, k, rows, :] = jnp.where(rock, pop[q, layer, rows, :], f[q])
                density, mz, my, mx = (part[side, k, rows, :] for k in range(4))
                arrived = add_all(f.values())
                density = density + arrived
                mz = mz + sign * arrived
                for q in enter:
                    _, ey, ex = LINKS[q]
                    if ey:
                        my = my + f[q] if ey == 1 else my - f[q]
                    if ex:
                        mx = mx + f[q] if ex == 1 else mx - f[q]
                relaxed = relax_solute(
                    [sol[q, layer, rows, :] for q in range(7)],
                    chem[0, layer, rows, :],
                    chem[1, layer, rows, :],
                    jnp.where(rock, 0.0, 1.0 / density),
                    (mz, my, mx),
                )
                into = slice(row, row + 8)
                for q in range(7):
                    faces[q, side, into, :] = relaxed[q]
                faces_moved[0, side, rows, :] = rolled(relaxed[5], 1)
                faces_moved[1, side, rows, :] = rolled(relaxed[6], -1)
                back = add_all(
                    streamed(q, outside, row, 8, shifted, plain, masks) for q in leave
                )
                base, partial, weight = (
                    ref[6 * span + k * width + 8 * t : 6 * span + k * width + 8 * t + 8, :]
                    for k in range(3)
                )
                cross_s[side, rows, :] = base + weight / (partial + back)
            for k, q in enumerate(enter):
                pltpu.make_async_copy(fbuf.at[side, k], flow.at[q, layer], sems.at[0]).start()
            for end, row, link in ((0, PAD - 1, 3), (1, PAD + width, 4)):
                at = 2 * end + side
                line = slice(at, at + 1)
                f = {q: streamed(q, layer, row, 1, shifted, plain, masks) for q in enter}
                density = edge_part[0, line, :] + add_all(f.values())
                my = edge_part[1, line, :]
                for q in enter:
                    if LINKS[q][1]:
                        my = my + f[q] if LINKS[q][1] == 1 else my - f[q]
                faces[link, side, row : row + 1, :] = edge_chem[0, line, :] + edge_chem[
                    1, line, :
                ] * (my / density)

        def solute_at(q, layer, row, count):
            if layer == 1:
                return middle[q, row : row + count, :]
            return faces[q, layer // 2, row : row + count, :]

        for layer in (1, 0, 2):
            for t in range(tiles):
                row, rows = PAD + 8 * t, slice(8 * t, 8 * t + 8)
                rock = pore[layer, rows, :] == 0
                for q in range(7):
                    ez, ey, ex = LINKS[q]
                    src = layer - ez
                    if src == -1:
                        v = cross_s[0, rows, :]
                    elif src == 3:
                        v = cross_s[1, rows, :]
                    elif ex and layer == 1:
                        v = middle_moved[q - 5, rows, :]
                    elif ex:
                        v = faces_moved[q - 5, layer // 2, rows, :]
                    else:
                        v = solute_at(q, src, row - ey, 8)
                    if q:
                        open_ = masks(ex, src, row - ey, 8) > 0.0
                        v = jnp.where(open_, v, solute_at(REVERSE[q], layer, row, 8))
                    sbuf[q, layer, rows, :] = jnp.where(rock, sol[q, layer, rows, :], v)
            pltpu.make_async_copy(sbuf.at[:, layer], solute.at[:, layer], sems.at[1]).start()

    by_parity(body, on_chip, across)
    pltpu.make_async_copy(outer_flow, flow.at[:, pl.ds(0, 2)], sems.at[0]).wait()
    pltpu.make_async_copy(sbuf, solute, sems.at[1]).wait()


VMEM = pl.BlockSpec(memory_space=pltpu.VMEM)
ANY = pl.BlockSpec(memory_space=pl.ANY)
HBM = pl.BlockSpec(memory_space=pltpu.HBM)
DMA = pltpu.SemaphoreType.DMA


def call(kernel, operands, specs, outs, scratch=(), aliases=None, flops=1_000_000):
    return pl.pallas_call(
        kernel,
        out_shape=[jax.ShapeDtypeStruct(s, jnp.float32) for s, _ in outs],
        in_specs=list(specs),
        out_specs=[spec for _, spec in outs],
        scratch_shapes=[pltpu.VMEM(s, jnp.float32) if isinstance(s, tuple) else s for s in scratch],
        input_output_aliases=aliases or {},
        compiler_params=pltpu.CompilerParams(vmem_limit_bytes=MAX_VMEM),
        cost_estimate=pl.CostEstimate(flops=flops, bytes_accessed=1_000_000, transcendentals=0),
        name=kernel.__name__,
    )(*operands)


def on_device(populations, solute, pore_mask, mineral_ids, reaction_rates, saturation):
    width = pore_mask.shape[1]
    padded = width + 2 * PAD
    cells = (populations, solute, pore_mask, mineral_ids)
    tables = (reaction_rates, saturation)
    gz, gy = lax.axis_size("gz"), lax.axis_size("gy")
    kinds = reaction_rates.shape
    first, second, table = call(
        pack_edges,
        tuple(pltpu.with_memory_space_constraint(v, pltpu.HBM) for v in cells + tables),
        [HBM] * 6,
        [((EDGE_ROWS, LX), VMEM)] * 2 + [((2 * kinds[0], LX), VMEM)],
        [
            (2, 19, 3, 8, LX),
            (2, 7, 3, 8, LX),
            pltpu.VMEM((2, 3, 8, LX), jnp.int32),
            pltpu.VMEM((2, 3, 8, LX), jnp.int32),
            (2, 3, NEAR, 8, LX),
            pltpu.SMEM(kinds, jnp.float32),
            pltpu.SMEM(kinds, jnp.float32),
            DMA((3,)),
        ],
    )
    def pairs(upward):
        found = []
        for place in range(gz * gy):
            ends = (place, place + 1)
            if ends[1] % gy:
                found.append(ends if upward == (place < gz // 2 * gy) else ends[::-1])
        return found

    first = lax.ppermute(first, ("gz", "gy"), pairs(True))
    second = lax.ppermute(second, ("gz", "gy"), pairs(False))
    whole = ((19, 3, padded, LX), VMEM)
    masks = ((3, 3, padded, LX), VMEM)
    moved, kept, mask, chem = call(
        relax_kernel,
        cells + (table,),
        [VMEM] * 5,
        [
            whole,
            whole,
            masks,
            ((2, 3, width, LX), VMEM),
        ],
        flops=6_000_000,
    )
    rows = 9 * width + 6 * SPAN
    moved, kept, mask, across, on_chip, edges = call(
        face_kernel,
        (moved, kept, mask, first, second, solute, chem),
        [VMEM] * 7,
        [
            whole,
            whole,
            masks,
            ((rows, LX), VMEM),
            ((rows, LX), VMEM),
            ((2, EDGE_ROWS, LX), VMEM),
        ],
        [(2, 2, EDGE_ROWS, LX)],
        {0: 0, 1: 1, 2: 2},
    )
    across = lax.ppermute(
        across, "gz", [(i, (i + 1 if i % 2 else i - 1) % gz) for i in range(gz)]
    )
    on_chip = lax.ppermute(on_chip, "gz", [(i, i + 1 - 2 * (i % 2)) for i in range(gz)])
    flow, outer_flow, part, edge_part, edge_chem, middle, middle_moved = call(
        inner_kernel,
        (populations, solute, pore_mask, chem, moved, kept, mask, edges, table),
        [VMEM] * 9,
        [
            (populations.shape, ANY),
            ((19, 2, width, LX), VMEM),
            ((2, 4, width, LX), VMEM),
            ((2, 8, LX), VMEM),
            ((2, 8, LX), VMEM),
            ((7, padded, LX), VMEM),
            ((2, width, LX), VMEM),
        ],
        [(19, width, LX), DMA],
        flops=6_000_000,
    )
    return tuple(
        call(
            outer_kernel,
            cells[:3]
            + (chem, moved, kept, mask, part, edge_part, edge_chem, middle, middle_moved)
            + (across, on_chip, outer_flow, flow),
            [VMEM] * 15 + [ANY],
            [(populations.shape, ANY), (solute.shape, ANY)],
            [
                (7, 2, padded, LX),
                (2, 2, width, LX),
                (2, width, LX),
                (2, 5, width, LX),
                (7, 3, width, LX),
                DMA((2,)),
            ],
            {15: 0},
        )
    )


def solution(mesh):
    cells = P(None, "gz", "gy", None)
    return jax.shard_map(
        on_device,
        mesh=mesh,
        in_specs=(cells, cells, P("gz", "gy", None), P("gz", "gy", None), P(), P()),
        out_specs=(cells, cells),
        check_vma=False,
    )
```

```python
import functools

import jax
import jax.numpy as jnp
import numpy as np
from jax import lax
from jax.experimental import pallas as pl
from jax.experimental.pallas import tpu as pltpu
from jax.sharding import PartitionSpec as P

LINKS = (
    (0, 0, 0),
    (1, 0, 0),
    (-1, 0, 0),
    (0, 1, 0),
    (0, -1, 0),
    (0, 0, 1),
    (0, 0, -1),
    (1, 1, 0),
    (-1, -1, 0),
    (1, -1, 0),
    (-1, 1, 0),
    (1, 0, 1),
    (-1, 0, -1),
    (1, 0, -1),
    (-1, 0, 1),
    (0, 1, 1),
    (0, -1, -1),
    (0, 1, -1),
    (0, -1, 1),
)
REVERSE = (0, 2, 1, 4, 3, 6, 5, 8, 7, 10, 9, 12, 11, 14, 13, 16, 15, 18, 17)
W19 = (1.0 / 3.0,) + (1.0 / 18.0,) * 6 + (1.0 / 36.0,) * 12
W7 = (0.25,) + (0.125,) * 6
UP = tuple(q for q in range(19) if LINKS[q][0] == 1)
DOWN = tuple(q for q in range(19) if LINKS[q][0] == -1)
KEEP = 1.0 - 1.0 / 1.25
GAIN = 1.0 / 1.25
KEEP_S = 1.0 - 1.0 / 1.4
GAIN_S = 1.0 / 1.4
LX = 128
PAD = 8
MAX_VMEM = 12 * 1024 * 1024
NEAR = 23
FAR_ROWS = 3 * NEAR
EDGE_ROWS = 88
SPAN = 4


def relax(p):
    d = {q: p[q] - p[q + 1] for q in range(1, 19, 2)}
    s = {q: p[q] + p[q + 1] for q in range(1, 19, 2)}
    density = p[0] + (
        ((s[1] + s[3]) + (s[5] + s[7])) + ((s[9] + s[11]) + (s[13] + s[15])) + s[17]
    )
    mz = (d[1] + d[7]) + (d[9] + d[11]) + d[13]
    my = (d[3] + d[7]) + (d[15] + d[17]) - d[9]
    mx = (d[5] + d[11]) + (d[15] - d[13]) - d[17]
    inverse = 1.0 / density
    uz, uy, ux = mz * inverse, my * inverse, mx * inverse
    rest = 1.0 - 1.5 * (uz * uz + uy * uy + ux * ux)
    out = [None] * 19
    scaled = {w: density * (GAIN * w) for w in set(W19)}
    out[0] = KEEP * p[0] + scaled[W19[0]] * rest
    along = {
        1: uz,
        3: uy,
        5: ux,
        7: uz + uy,
        9: uz - uy,
        11: uz + ux,
        13: uz - ux,
        15: uy + ux,
        17: uy - ux,
    }
    for q, e in along.items():
        w = scaled[W19[q]]
        even = w * (rest + 4.5 * (e * e))
        odd = w * (3.0 * e)
        out[q] = KEEP * p[q] + (even + odd)
        out[q + 1] = KEEP * p[q + 1] + (even - odd)
    return out


def pick(ids, table):
    kinds = table.shape[0] // 2
    rate, goal = table[0:1, :], table[kinds : kinds + 1, :]
    for k in range(1, kinds):
        rate = jnp.where(ids == k, table[k : k + 1, :], rate)
        goal = jnp.where(ids == k, table[kinds + k : kinds + k + 1, :], goal)
    return rate, goal


def solute_terms(s, pore, ids, table):
    total = ((s[0] + s[1]) + (s[2] + s[3])) + ((s[4] + s[5]) + s[6])
    rate, goal = pick(ids, table)
    return total, jnp.where(pore == 2, -rate * (total - goal), 0.0)


def rolled(value, shift):
    return value if shift == 0 else pltpu.roll(value, shift % LX, axis=1)


def sums(f):
    d = {q: f[q] - f[q + 1] for q in range(1, 19, 2)}
    s = {q: f[q] + f[q + 1] for q in range(1, 19, 2)}
    density = f[0] + (
        ((s[1] + s[3]) + (s[5] + s[7])) + ((s[9] + s[11]) + (s[13] + s[15])) + s[17]
    )
    mz = (d[1] + d[7]) + (d[9] + d[11]) + d[13]
    my = (d[3] + d[7]) + (d[15] + d[17]) - d[9]
    mx = (d[5] + d[11]) + (d[15] - d[13]) - d[17]
    return density, mz, my, mx


def add_all(values):
    values = list(values)
    while len(values) > 1:
        values = [
            values[i] + values[i + 1] if i + 1 < len(values) else values[i]
            for i in range(0, len(values), 2)
        ]
    return values[0]


def toward(sign):
    return tuple(q for q in range(19) if LINKS[q][1] == sign)


def either(condition, when_true, when_false):
    pl.when(condition)(when_true)
    pl.when(jnp.logical_not(condition))(when_false)


def upper_half():
    return lax.axis_index("gz") >= lax.axis_size("gz") // 2


def by_parity(body, first, second):
    even = lax.rem(lax.axis_index("gz"), 2) == 0
    either(even, lambda: body(first, second), lambda: body(second, first))


def pack_edges(
    pop,
    sol,
    pore,
    ids,
    rates,
    target,
    first,
    second,
    table,
    epop,
    esol,
    epore,
    eids,
    erel,
    srates,
    starget,
    sems,
):
    width = pop.shape[2]
    for side, start, to in ((0, width - 2, 6), (1, 0, 0)):
        rows, into = pl.ds(start, 2), pl.ds(to, 2)
        for src, dst in (
            (pop.at[:, :, rows, :], epop.at[side, :, :, into, :]),
            (sol.at[:, :, rows, :], esol.at[side, :, :, into, :]),
            (pore.at[:, rows, :], epore.at[side, :, into, :]),
            (ids.at[:, rows, :], eids.at[side, :, into, :]),
        ):
            pltpu.make_async_copy(src, dst, sems.at[0]).start()
    constants = [
        pltpu.make_async_copy(rates, srates, sems.at[1]),
        pltpu.make_async_copy(target, starget, sems.at[2]),
    ]
    for copy in constants:
        copy.start()
    every = erel.at[0, :, pl.ds(0, 14)]
    pltpu.make_async_copy(every, every, sems.at[0]).wait()
    for copy in constants:
        copy.wait()
    for side, link in ((0, 3), (1, 4)):
        for layer in range(3):
            rel = relax([epop[side, q, layer] for q in range(19)])
            for q in range(19):
                erel[side, layer, q] = rel[q]
            kind = epore[side, layer].astype(jnp.float32)
            erel[side, layer, 19] = kind
            erel[side, layer, 20] = eids[side, layer].astype(jnp.float32)
            erel[side, layer, 21] = add_all(esol[side, q, layer] for q in range(7))
            erel[side, layer, 22] = esol[side, link, layer]

    def emit(up, down):
        for side, out, near, far, sign in ((0, up, 7, 6, 1), (1, down, 0, 1, -1)):
            for layer in range(3):
                for k in range(NEAR):
                    at = 3 * k + layer
                    out[at : at + 1, :] = erel[side, layer, k, near : near + 1, :]
                for k, q in enumerate(toward(sign) + (19,)):
                    at = FAR_ROWS + 3 * k + layer
                    out[at : at + 1, :] = erel[side, layer, q, far : far + 1, :]
            out[EDGE_ROWS - 1 : EDGE_ROWS, :] = jnp.zeros((1, LX), jnp.float32)

    either(upper_half(), lambda: emit(second, first), lambda: emit(first, second))
    kinds = srates.shape[0]
    for k in range(kinds):
        for at, ref in ((k, srates), (k + kinds, starget)):
            table[at : at + 1, :] = jnp.full((1, LX), ref[k], jnp.float32)


def face_payload(sol, chem, moved, kept, mask, across, on_chip, tiles, at_edges):
    width = sol.shape[2]
    span = width + SPAN
    shifted, plain, masks = readers(moved, kept, mask)

    def emit(up, down):
        for out, layer, cross, link in ((up, 2, UP, 1), (down, 0, DOWN, 2)):
            w = W7[link]
            for t in tiles:
                row, rows = PAD + 8 * t, slice(8 * t, 8 * t + 8)
                get = functools.partial(
                    streamed,
                    layer=layer,
                    row=row,
                    count=8,
                    shifted=shifted,
                    plain=plain,
                    masks=masks,
                )
                away = add_all(get(q) for q in cross)
                level = add_all(get(q) for q in range(19) if LINKS[q][0] == 0)
                partial = level + away
                total, reaction = chem[0, layer, rows, :], chem[1, layer, rows, :]
                slope = (4.0 * w * GAIN_S) * total
                base = KEEP_S * sol[link, layer, rows, :] + (w * GAIN_S) * total + w * reaction
                for k, v in enumerate((base - slope, partial, slope * (partial + away))):
                    at = 6 * span + k * width + 8 * t
                    out[at : at + 8, :] = v
            if at_edges:
                pieces = [(PAD - 2, 2, 0), (PAD + width, 2, 2 + width)]
            else:
                pieces = [(PAD + 8 * t, 8, 2 + 8 * t) for t in range(width // 8)]
            for k in range(6):
                for row, count, to in pieces:
                    v = plain(cross[k], layer, row, count) if k < 5 else masks(0, layer, row, count)
                    out[k * span + to : k * span + to + count, :] = v

    by_parity(emit, on_chip, across)


def relax_kernel(pop, sol, pore, ids, table, moved, kept, mask, chem, across, on_chip):
    width = pop.shape[2]
    for layer in range(3):
        for t in range(width // 8):
            rows, into = slice(8 * t, 8 * t + 8), slice(PAD + 8 * t, PAD + 8 * t + 8)
            out = relax([pop[q, layer, rows, :] for q in range(19)])
            for q in range(19):
                ex = LINKS[q][2]
                moved[q, layer, into, :] = rolled(out[q], ex)
                if ex:
                    kept[q, layer, into, :] = out[q]
            kind = pore[layer, rows, :]
            m = jnp.where(kind > 0, 1.0, 0.0)
            for ex in (0, 1, -1):
                mask[ex % 3, layer, into, :] = rolled(m, ex)
            s = [sol[q, layer, rows, :] for q in range(7)]
            total, reaction = solute_terms(s, kind, ids[layer, rows, :], table)
            chem[0, layer, rows, :] = total
            chem[1, layer, rows, :] = reaction
    face_payload(
        sol, chem, moved, kept, mask, across, on_chip, range(1, width // 8 - 1), False
    )


def streamed(q, layer, row, count, shifted, plain, masks):
    ez, ey, ex = LINKS[q]
    value = shifted(q, layer - ez, row - ey, count)
    if q == 0:
        return value
    open_ = masks(ex, layer - ez, row - ey, count) > 0.0
    return jnp.where(open_, value, plain(REVERSE[q], layer, row, count))


def readers(moved, kept, mask):
    def shifted(q, layer, row, count):
        return moved[q, layer, row : row + count, :]

    def plain(q, layer, row, count):
        return (kept if LINKS[q][2] else moved)[q, layer, row : row + count, :]

    def masks(ex, layer, row, count):
        return mask[ex % 3, layer, row : row + count, :]

    return shifted, plain, masks


def face_kernel(
    moved_in,
    kept_in,
    mask_in,
    across_in,
    on_chip_in,
    first,
    second,
    sol,
    chem,
    moved,
    kept,
    mask,
    across,
    on_chip,
    edges,
    turned,
):
    del moved_in, kept_in, mask_in, across_in, on_chip_in
    width = sol.shape[2]
    upper = upper_half()
    for t in range(EDGE_ROWS // 8):
        rows = slice(8 * t, 8 * t + 8)
        for side, v in (
            (0, jnp.where(upper, second[rows, :], first[rows, :])),
            (1, jnp.where(upper, first[rows, :], second[rows, :])),
        ):
            edges[side, rows, :] = v
            turned[side, 0, rows, :] = rolled(v, 1)
            turned[side, 1, rows, :] = rolled(v, -1)
    for side, near, far, sign in (
        (0, PAD - 1, PAD - 2, 1),
        (1, PAD + width, PAD + width + 1, -1),
    ):

        def line(at, ex):
            if ex == 0:
                return edges[side, at : at + 1, :]
            return turned[side, 0 if ex == 1 else 1, at : at + 1, :]

        for layer in range(3):
            for row, start, links in (
                (near, 0, tuple(range(19))),
                (far, FAR_ROWS, toward(sign)),
            ):
                into = slice(row, row + 1)
                for k, q in enumerate(links):
                    at, ex = start + 3 * k + layer, LINKS[q][2]
                    moved[q, layer, into, :] = line(at, ex)
                    if ex:
                        kept[q, layer, into, :] = line(at, 0)
                at = start + 3 * len(links) + layer
                for ex in (0, 1, -1):
                    mask[ex % 3, layer, into, :] = line(at, ex)
    face_payload(sol, chem, moved, kept, mask, across, on_chip, (0, width // 8 - 1), True)


def inner_kernel(
    pop,
    sol,
    pore,
    chem,
    moved,
    kept,
    mask,
    edges,
    table,
    flow,
    outer_flow,
    part,
    edge_part,
    edge_chem,
    middle,
    middle_moved,
    buffer,
    sem,
):
    width = pop.shape[2]
    tiles = width // 8
    shifted, plain, masks = readers(moved, kept, mask)
    zero8 = jnp.zeros((8, LX), jnp.float32)
    zero1 = jnp.zeros((1, LX), jnp.float32)

    def pull(layer, row, count, zero):
        return [
            streamed(q, layer, row, count, shifted, plain, masks)
            if 0 <= layer - LINKS[q][0] <= 2
            else zero
            for q in range(19)
        ]

    for layer in (1, 0, 2):
        for t in range(tiles):
            row, rows = PAD + 8 * t, slice(8 * t, 8 * t + 8)
            f = pull(layer, row, 8, zero8)
            rock = pore[layer, rows, :] == 0
            for q in range(19):
                if 0 <= layer - LINKS[q][0] <= 2:
                    v = jnp.where(rock, pop[q, layer, rows, :], f[q])
                    if layer == 1:
                        buffer[q, rows, :] = v
                    else:
                        outer_flow[q, layer // 2, rows, :] = v
            density, mz, my, mx = sums(f)
            if layer != 1:
                for k, v in enumerate((density, mz, my, mx)):
                    part[layer // 2, k, rows, :] = v
                continue
            relaxed = relax_solute(
                [sol[q, layer, rows, :] for q in range(7)],
                chem[0, layer, rows, :],
                chem[1, layer, rows, :],
                jnp.where(rock, 0.0, 1.0 / density),
                (mz, my, mx),
            )
            into = slice(row, row + 8)
            for q in range(7):
                middle[q, into, :] = relaxed[q]
            middle_moved[0, rows, :] = rolled(relaxed[5], 1)
            middle_moved[1, rows, :] = rolled(relaxed[6], -1)
        if layer == 1:
            copy = pltpu.make_async_copy(buffer, flow.at[:, 1], sem)
            copy.start()
    for side, row, link, sign in ((0, PAD - 1, 3, 1.0), (1, PAD + width, 4, -1.0)):
        w = W7[link]
        for layer in range(3):
            kind, mineral, total, own = (
                edges[side, 3 * k + layer : 3 * k + layer + 1, :] for k in range(19, 23)
            )
            rate, goal = pick(mineral, table)
            reaction = jnp.where(kind == 2.0, -rate * (total - goal), 0.0)
            base = KEEP_S * own + (w * GAIN_S) * total + w * reaction
            slope = (sign * 4.0 * w * GAIN_S) * total
            density, _, my, _ = sums(pull(layer, row, 1, zero1))
            if layer == 1:
                middle[link, row : row + 1, :] = base + slope * (my / density)
            else:
                at = 2 * side + layer // 2
                edge_part[0, at : at + 1, :] = density
                edge_part[1, at : at + 1, :] = my
                edge_chem[0, at : at + 1, :] = base
                edge_chem[1, at : at + 1, :] = slope
    copy.wait()


def relax_solute(s, total, reaction, inverse, momenta):
    common = (W7[1] * GAIN_S) * total + W7[1] * reaction
    slope = (4.0 * W7[1] * GAIN_S) * total * inverse
    out = [KEEP_S * s[0] + (W7[0] * GAIN_S) * total + W7[0] * reaction]
    for q, m in zip((1, 3, 5), momenta):
        out.append(KEEP_S * s[q] + common + slope * m)
        out.append(KEEP_S * s[q + 1] + common - slope * m)
    return out


def outer_kernel(
    pop,
    sol,
    pore,
    chem,
    moved,
    kept,
    mask,
    part,
    edge_part,
    edge_chem,
    middle,
    middle_moved,
    across,
    on_chip,
    outer_flow,
    flow_in,
    flow,
    solute,
    faces,
    faces_moved,
    cross_s,
    fbuf,
    sbuf,
    sems,
):
    del flow_in
    width = pop.shape[2]
    tiles = width // 8
    span = width + SPAN
    own = readers(moved, kept, mask)
    for layer in (0, 2):
        local = [q for q in range(19) if 0 <= layer - LINKS[q][0] <= 2]
        start = 0
        while start < len(local):
            stop = start
            while stop + 1 < len(local) and local[stop + 1] == local[stop] + 1:
                stop += 1
            links = pl.ds(local[start], local[stop] - local[start] + 1)
            pltpu.make_async_copy(
                outer_flow.at[links, layer // 2], flow.at[links, layer], sems.at[0]
            ).start()
            start = stop + 1

    def body(above, below):
        def value(q, layer, row, count):
            ref, links = (below, UP) if layer == -1 else (above, DOWN)
            at = links.index(q) * span + row - PAD + 2
            return ref[at : at + count, :]

        def shifted(q, layer, row, count):
            if 0 <= layer <= 2:
                return own[0](q, layer, row, count)
            return rolled(value(q, layer, row, count), LINKS[q][2])

        def plain(q, layer, row, count):
            if 0 <= layer <= 2:
                return own[1](q, layer, row, count)
            return value(q, layer, row, count)

        def masks(ex, layer, row, count):
            if 0 <= layer <= 2:
                return own[2](ex, layer, row, count)
            at = 5 * span + row - PAD + 2
            return rolled((below if layer == -1 else above)[at : at + count, :], ex)

        for side, ref, layer, outside, enter, leave in (
            (0, below, 0, -1, UP, DOWN),
            (1, above, 2, 3, DOWN, UP),
        ):
            sign = 1.0 if side == 0 else -1.0
            for t in range(tiles):
                row, rows = PAD + 8 * t, slice(8 * t, 8 * t + 8)
                rock = pore[layer, rows, :] == 0
                f = {q: streamed(q, layer, row, 8, shifted, plain, masks) for q in enter}
                for k, q in enumerate(enter):
                    fbuf[side, k, rows, :] = jnp.where(rock, pop[q, layer, rows, :], f[q])
                density, mz, my, mx = (part[side, k, rows, :] for k in range(4))
                arrived = add_all(f.values())
                density = density + arrived
                mz = mz + sign * arrived
                for q in enter:
                    _, ey, ex = LINKS[q]
                    if ey:
                        my = my + f[q] if ey == 1 else my - f[q]
                    if ex:
                        mx = mx + f[q] if ex == 1 else mx - f[q]
                relaxed = relax_solute(
                    [sol[q, layer, rows, :] for q in range(7)],
                    chem[0, layer, rows, :],
                    chem[1, layer, rows, :],
                    jnp.where(rock, 0.0, 1.0 / density),
                    (mz, my, mx),
                )
                into = slice(row, row + 8)
                for q in range(7):
                    faces[q, side, into, :] = relaxed[q]
                faces_moved[0, side, rows, :] = rolled(relaxed[5], 1)
                faces_moved[1, side, rows, :] = rolled(relaxed[6], -1)
                back = add_all(
                    streamed(q, outside, row, 8, shifted, plain, masks) for q in leave
                )
                base, partial, weight = (
                    ref[6 * span + k * width + 8 * t : 6 * span + k * width + 8 * t + 8, :]
                    for k in range(3)
                )
                cross_s[side, rows, :] = base + weight / (partial + back)
            for k, q in enumerate(enter):
                pltpu.make_async_copy(fbuf.at[side, k], flow.at[q, layer], sems.at[0]).start()
            for end, row, link in ((0, PAD - 1, 3), (1, PAD + width, 4)):
                at = 2 * end + side
                line = slice(at, at + 1)
                f = {q: streamed(q, layer, row, 1, shifted, plain, masks) for q in enter}
                density = edge_part[0, line, :] + add_all(f.values())
                my = edge_part[1, line, :]
                for q in enter:
                    if LINKS[q][1]:
                        my = my + f[q] if LINKS[q][1] == 1 else my - f[q]
                faces[link, side, row : row + 1, :] = edge_chem[0, line, :] + edge_chem[
                    1, line, :
                ] * (my / density)

        def solute_at(q, layer, row, count):
            if layer == 1:
                return middle[q, row : row + count, :]
            return faces[q, layer // 2, row : row + count, :]

        for layer in (1, 0, 2):
            for t in range(tiles):
                row, rows = PAD + 8 * t, slice(8 * t, 8 * t + 8)
                rock = pore[layer, rows, :] == 0
                for q in range(7):
                    ez, ey, ex = LINKS[q]
                    src = layer - ez
                    if src == -1:
                        v = cross_s[0, rows, :]
                    elif src == 3:
                        v = cross_s[1, rows, :]
                    elif ex and layer == 1:
                        v = middle_moved[q - 5, rows, :]
                    elif ex:
                        v = faces_moved[q - 5, layer // 2, rows, :]
                    else:
                        v = solute_at(q, src, row - ey, 8)
                    if q:
                        open_ = masks(ex, src, row - ey, 8) > 0.0
                        v = jnp.where(open_, v, solute_at(REVERSE[q], layer, row, 8))
                    sbuf[q, layer, rows, :] = jnp.where(rock, sol[q, layer, rows, :], v)
            pltpu.make_async_copy(sbuf.at[:, layer], solute.at[:, layer], sems.at[1]).start()

    by_parity(body, on_chip, across)
    pltpu.make_async_copy(outer_flow, flow.at[:, pl.ds(0, 2)], sems.at[0]).wait()
    pltpu.make_async_copy(sbuf, solute, sems.at[1]).wait()


VMEM = pl.BlockSpec(memory_space=pltpu.VMEM)
ANY = pl.BlockSpec(memory_space=pl.ANY)
HBM = pl.BlockSpec(memory_space=pltpu.HBM)
DMA = pltpu.SemaphoreType.DMA


def call(kernel, operands, specs, outs, scratch=(), aliases=None, flops=1_000_000):
    return pl.pallas_call(
        kernel,
        out_shape=[jax.ShapeDtypeStruct(s, jnp.float32) for s, _ in outs],
        in_specs=list(specs),
        out_specs=[spec for _, spec in outs],
        scratch_shapes=[pltpu.VMEM(s, jnp.float32) if isinstance(s, tuple) else s for s in scratch],
        input_output_aliases=aliases or {},
        compiler_params=pltpu.CompilerParams(vmem_limit_bytes=MAX_VMEM),
        cost_estimate=pl.CostEstimate(flops=flops, bytes_accessed=1_000_000, transcendentals=0),
        name=kernel.__name__,
    )(*operands)


def on_device(populations, solute, pore_mask, mineral_ids, reaction_rates, saturation):
    width = pore_mask.shape[1]
    padded = width + 2 * PAD
    cells = (populations, solute, pore_mask, mineral_ids)
    tables = (reaction_rates, saturation)
    gz, gy = lax.axis_size("gz"), lax.axis_size("gy")
    kinds = reaction_rates.shape
    first, second, table = call(
        pack_edges,
        tuple(pltpu.with_memory_space_constraint(v, pltpu.HBM) for v in cells + tables),
        [HBM] * 6,
        [((EDGE_ROWS, LX), VMEM)] * 2 + [((2 * kinds[0], LX), VMEM)],
        [
            (2, 19, 3, 8, LX),
            (2, 7, 3, 8, LX),
            pltpu.VMEM((2, 3, 8, LX), jnp.int32),
            pltpu.VMEM((2, 3, 8, LX), jnp.int32),
            (2, 3, NEAR, 8, LX),
            pltpu.SMEM(kinds, jnp.float32),
            pltpu.SMEM(kinds, jnp.float32),
            DMA((3,)),
        ],
    )
    def pairs(upward):
        found = []
        for place in range(gz * gy):
            ends = (place, place + 1)
            if ends[1] % gy:
                found.append(ends if upward == (place < gz // 2 * gy) else ends[::-1])
        return found

    first = lax.ppermute(first, ("gz", "gy"), pairs(True))
    second = lax.ppermute(second, ("gz", "gy"), pairs(False))
    rows = 9 * width + 6 * SPAN
    whole = ((19, 3, padded, LX), VMEM)
    masks = ((3, 3, padded, LX), VMEM)
    moved, kept, mask, chem, across, on_chip = call(
        relax_kernel,
        cells + (table,),
        [VMEM] * 5,
        [
            whole,
            whole,
            masks,
            ((2, 3, width, LX), VMEM),
            ((rows, LX), VMEM),
            ((rows, LX), VMEM),
        ],
        flops=6_000_000,
    )
    moved, kept, mask, across, on_chip, edges = call(
        face_kernel,
        (moved, kept, mask, across, on_chip, first, second, solute, chem),
        [VMEM] * 9,
        [
            whole,
            whole,
            masks,
            ((rows, LX), VMEM),
            ((rows, LX), VMEM),
            ((2, EDGE_ROWS, LX), VMEM),
        ],
        [(2, 2, EDGE_ROWS, LX)],
        {k: k for k in range(5)},
    )
    across = lax.ppermute(
        across, "gz", [(i, (i + 1 if i % 2 else i - 1) % gz) for i in range(gz)]
    )
    on_chip = lax.ppermute(on_chip, "gz", [(i, i + 1 - 2 * (i % 2)) for i in range(gz)])
    flow, outer_flow, part, edge_part, edge_chem, middle, middle_moved = call(
        inner_kernel,
        (populations, solute, pore_mask, chem, moved, kept, mask, edges, table),
        [VMEM] * 9,
        [
            (populations.shape, ANY),
            ((19, 2, width, LX), VMEM),
            ((2, 4, width, LX), VMEM),
            ((2, 8, LX), VMEM),
            ((2, 8, LX), VMEM),
            ((7, padded, LX), VMEM),
            ((2, width, LX), VMEM),
        ],
        [(19, width, LX), DMA],
        flops=6_000_000,
    )
    return tuple(
        call(
            outer_kernel,
            cells[:3]
            + (chem, moved, kept, mask, part, edge_part, edge_chem, middle, middle_moved)
            + (across, on_chip, outer_flow, flow),
            [VMEM] * 15 + [ANY],
            [(populations.shape, ANY), (solute.shape, ANY)],
            [
                (7, 2, padded, LX),
                (2, 2, width, LX),
                (2, width, LX),
                (2, 5, width, LX),
                (7, 3, width, LX),
                DMA((2,)),
            ],
            {15: 0},
        )
    )


def solution(mesh):
    cells = P(None, "gz", "gy", None)
    return jax.shard_map(
        on_device,
        mesh=mesh,
        in_specs=(cells, cells, P("gz", "gy", None), P("gz", "gy", None), P(), P()),
        out_specs=(cells, cells),
        check_vma=False,
    )
```

```python
import functools

import jax
import jax.numpy as jnp
import numpy as np
from jax import lax
from jax.experimental import pallas as pl
from jax.experimental.pallas import tpu as pltpu
from jax.sharding import PartitionSpec as P

LINKS = (
    (0, 0, 0),
    (1, 0, 0),
    (-1, 0, 0),
    (0, 1, 0),
    (0, -1, 0),
    (0, 0, 1),
    (0, 0, -1),
    (1, 1, 0),
    (-1, -1, 0),
    (1, -1, 0),
    (-1, 1, 0),
    (1, 0, 1),
    (-1, 0, -1),
    (1, 0, -1),
    (-1, 0, 1),
    (0, 1, 1),
    (0, -1, -1),
    (0, 1, -1),
    (0, -1, 1),
)
REVERSE = (0, 2, 1, 4, 3, 6, 5, 8, 7, 10, 9, 12, 11, 14, 13, 16, 15, 18, 17)
W19 = (1.0 / 3.0,) + (1.0 / 18.0,) * 6 + (1.0 / 36.0,) * 12
W7 = (0.25,) + (0.125,) * 6
UP = tuple(q for q in range(19) if LINKS[q][0] == 1)
DOWN = tuple(q for q in range(19) if LINKS[q][0] == -1)
KEEP = 1.0 - 1.0 / 1.25
GAIN = 1.0 / 1.25
KEEP_S = 1.0 - 1.0 / 1.4
GAIN_S = 1.0 / 1.4
LX = 128
PAD = 8
MAX_VMEM = 12 * 1024 * 1024
NEAR = 23
FAR_ROWS = 3 * NEAR
EDGE_ROWS = 88


def relax(p):
    d = {q: p[q] - p[q + 1] for q in range(1, 19, 2)}
    s = {q: p[q] + p[q + 1] for q in range(1, 19, 2)}
    density = p[0] + (
        ((s[1] + s[3]) + (s[5] + s[7])) + ((s[9] + s[11]) + (s[13] + s[15])) + s[17]
    )
    mz = (d[1] + d[7]) + (d[9] + d[11]) + d[13]
    my = (d[3] + d[7]) + (d[15] + d[17]) - d[9]
    mx = (d[5] + d[11]) + (d[15] - d[13]) - d[17]
    inverse = 1.0 / density
    uz, uy, ux = mz * inverse, my * inverse, mx * inverse
    rest = 1.0 - 1.5 * (uz * uz + uy * uy + ux * ux)
    out = [None] * 19
    scaled = {w: density * (GAIN * w) for w in set(W19)}
    out[0] = KEEP * p[0] + scaled[W19[0]] * rest
    along = {
        1: uz,
        3: uy,
        5: ux,
        7: uz + uy,
        9: uz - uy,
        11: uz + ux,
        13: uz - ux,
        15: uy + ux,
        17: uy - ux,
    }
    for q, e in along.items():
        w = scaled[W19[q]]
        even = w * (rest + 4.5 * (e * e))
        odd = w * (3.0 * e)
        out[q] = KEEP * p[q] + (even + odd)
        out[q + 1] = KEEP * p[q + 1] + (even - odd)
    return out


def pick(ids, table):
    kinds = table.shape[0] // 2
    rate, goal = table[0:1, :], table[kinds : kinds + 1, :]
    for k in range(1, kinds):
        rate = jnp.where(ids == k, table[k : k + 1, :], rate)
        goal = jnp.where(ids == k, table[kinds + k : kinds + k + 1, :], goal)
    return rate, goal


def solute_terms(s, pore, ids, table):
    total = ((s[0] + s[1]) + (s[2] + s[3])) + ((s[4] + s[5]) + s[6])
    rate, goal = pick(ids, table)
    return total, jnp.where(pore == 2, -rate * (total - goal), 0.0)


def rolled(value, shift):
    return value if shift == 0 else pltpu.roll(value, shift % LX, axis=1)


def sums(f):
    d = {q: f[q] - f[q + 1] for q in range(1, 19, 2)}
    s = {q: f[q] + f[q + 1] for q in range(1, 19, 2)}
    density = f[0] + (
        ((s[1] + s[3]) + (s[5] + s[7])) + ((s[9] + s[11]) + (s[13] + s[15])) + s[17]
    )
    mz = (d[1] + d[7]) + (d[9] + d[11]) + d[13]
    my = (d[3] + d[7]) + (d[15] + d[17]) - d[9]
    mx = (d[5] + d[11]) + (d[15] - d[13]) - d[17]
    return density, mz, my, mx


def add_all(values):
    values = list(values)
    while len(values) > 1:
        values = [
            values[i] + values[i + 1] if i + 1 < len(values) else values[i]
            for i in range(0, len(values), 2)
        ]
    return values[0]


def toward(sign):
    return tuple(q for q in range(19) if LINKS[q][1] == sign)


def either(condition, when_true, when_false):
    pl.when(condition)(when_true)
    pl.when(jnp.logical_not(condition))(when_false)


def upper_half():
    return lax.axis_index("gz") >= lax.axis_size("gz") // 2


def by_parity(body, first, second):
    even = lax.rem(lax.axis_index("gz"), 2) == 0
    either(even, lambda: body(first, second), lambda: body(second, first))


def pack_edges(
    pop,
    sol,
    pore,
    ids,
    rates,
    target,
    first,
    second,
    table,
    epop,
    esol,
    epore,
    eids,
    erel,
    srates,
    starget,
    sems,
):
    width = pop.shape[2]
    for side, start in ((0, width - 2), (1, 0)):
        rows = pl.ds(start, 2)
        for layer in range(3):
            into = pl.ds(2 * layer, 2)
            for src, dst in (
                (pop.at[:, layer, rows, :], epop.at[side, :, into, :]),
                (sol.at[:, layer, rows, :], esol.at[side, :, into, :]),
                (pore.at[layer, rows, :], epore.at[side, into, :]),
                (ids.at[layer, rows, :], eids.at[side, into, :]),
            ):
                pltpu.make_async_copy(src, dst, sems.at[0]).start()
    constants = [
        pltpu.make_async_copy(rates, srates, sems.at[1]),
        pltpu.make_async_copy(target, starget, sems.at[2]),
    ]
    for copy in constants:
        copy.start()
    every = erel.at[:, pl.ds(0, 21)]
    pltpu.make_async_copy(every, every, sems.at[0]).wait()
    for copy in constants:
        copy.wait()
    for side, link in ((0, 3), (1, 4)):
        rel = relax([epop[side, q] for q in range(19)])
        for q in range(19):
            erel[side, q] = rel[q]
        erel[side, 19] = epore[side].astype(jnp.float32)
        erel[side, 20] = eids[side].astype(jnp.float32)
        erel[side, 21] = add_all(esol[side, q] for q in range(7))
        erel[side, 22] = esol[side, link]

    def emit(up, down):
        for side, out, near, far, sign in ((0, up, 1, 0, 1), (1, down, 0, 1, -1)):
            for layer in range(3):
                row = 2 * layer + near
                for k in range(NEAR):
                    at = 3 * k + layer
                    out[at : at + 1, :] = erel[side, k, row : row + 1, :]
                row = 2 * layer + far
                for k, q in enumerate(toward(sign) + (19,)):
                    at = FAR_ROWS + 3 * k + layer
                    out[at : at + 1, :] = erel[side, q, row : row + 1, :]
            out[EDGE_ROWS - 1 : EDGE_ROWS, :] = jnp.zeros((1, LX), jnp.float32)

    either(upper_half(), lambda: emit(second, first), lambda: emit(first, second))
    kinds = srates.shape[0]
    for k in range(kinds):
        for at, ref in ((k, srates), (k + kinds, starget)):
            table[at : at + 1, :] = jnp.full((1, LX), ref[k], jnp.float32)


def place(k, links, row, width):
    if k == 5:
        return 5 * (width + 2) + row - (PAD - 2)
    return k * (width + 2) + row - (PAD - 1 - LINKS[links[k]][1])


def field(k, row, width):
    return 6 * width + 14 + k * width + row - PAD


def face_payload(sol, chem, moved, kept, mask, across, on_chip, tiles, at_edges):
    width = sol.shape[2]
    shifted, plain, masks = readers(moved, kept, mask)

    def emit(up, down):
        for out, layer, cross, link in ((up, 2, UP, 1), (down, 0, DOWN, 2)):
            w = W7[link]
            for t in tiles:
                row, rows = PAD + 8 * t, slice(8 * t, 8 * t + 8)
                get = functools.partial(
                    streamed,
                    layer=layer,
                    row=row,
                    count=8,
                    shifted=shifted,
                    plain=plain,
                    masks=masks,
                )
                away = add_all(get(q) for q in cross)
                level = add_all(get(q) for q in range(19) if LINKS[q][0] == 0)
                partial = level + away
                total, reaction = chem[0, layer, rows, :], chem[1, layer, rows, :]
                slope = (4.0 * w * GAIN_S) * total
                base = KEEP_S * sol[link, layer, rows, :] + (w * GAIN_S) * total + w * reaction
                for k, v in enumerate((base - slope, partial, slope * (partial + away))):
                    at = field(k, row, width)
                    out[at : at + 8, :] = v
            for k in range(6):
                ey = LINKS[cross[k]][1] if k < 5 else 0
                extra = 2 if k == 5 else 1
                below, above = extra + ey, extra - ey
                pieces = [(PAD + 8 * t, 8) for t in range(width // 8)]
                if at_edges:
                    pieces = [(PAD - below, below), (PAD + width, above)]
                for row, count in pieces:
                    if count:
                        at = place(k, cross, row, width)
                        v = plain(cross[k], layer, row, count) if k < 5 else masks(0, layer, row, count)
                        out[at : at + count, :] = v

    by_parity(emit, on_chip, across)


def relax_kernel(pop, sol, pore, ids, table, moved, kept, mask, chem, across, on_chip):
    width = pop.shape[2]
    for layer in range(3):
        for t in range(width // 8):
            rows, into = slice(8 * t, 8 * t + 8), slice(PAD + 8 * t, PAD + 8 * t + 8)
            out = relax([pop[q, layer, rows, :] for q in range(19)])
            for q in range(19):
                ex = LINKS[q][2]
                moved[q, layer, into, :] = rolled(out[q], ex)
                if ex:
                    kept[q, layer, into, :] = out[q]
            kind = pore[layer, rows, :]
            m = jnp.where(kind > 0, 1.0, 0.0)
            for ex in (0, 1, -1):
                mask[ex % 3, layer, into, :] = rolled(m, ex)
            s = [sol[q, layer, rows, :] for q in range(7)]
            total, reaction = solute_terms(s, kind, ids[layer, rows, :], table)
            chem[0, layer, rows, :] = total
            chem[1, layer, rows, :] = reaction
    face_payload(
        sol, chem, moved, kept, mask, across, on_chip, range(1, width // 8 - 1), False
    )


def streamed(q, layer, row, count, shifted, plain, masks):
    ez, ey, ex = LINKS[q]
    value = shifted(q, layer - ez, row - ey, count)
    if q == 0:
        return value
    open_ = masks(ex, layer - ez, row - ey, count) > 0.0
    return jnp.where(open_, value, plain(REVERSE[q], layer, row, count))


def readers(moved, kept, mask):
    def shifted(q, layer, row, count):
        return moved[q, layer, row : row + count, :]

    def plain(q, layer, row, count):
        return (kept if LINKS[q][2] else moved)[q, layer, row : row + count, :]

    def masks(ex, layer, row, count):
        return mask[ex % 3, layer, row : row + count, :]

    return shifted, plain, masks


def face_kernel(
    moved_in,
    kept_in,
    mask_in,
    across_in,
    on_chip_in,
    first,
    second,
    sol,
    chem,
    moved,
    kept,
    mask,
    across,
    on_chip,
    edges,
    turned,
):
    del moved_in, kept_in, mask_in, across_in, on_chip_in
    width = sol.shape[2]
    upper = upper_half()
    for t in range(EDGE_ROWS // 8):
        rows = slice(8 * t, 8 * t + 8)
        for side, v in (
            (0, jnp.where(upper, second[rows, :], first[rows, :])),
            (1, jnp.where(upper, first[rows, :], second[rows, :])),
        ):
            edges[side, rows, :] = v
            turned[side, 0, rows, :] = rolled(v, 1)
            turned[side, 1, rows, :] = rolled(v, -1)
    for side, near, far, sign in (
        (0, PAD - 1, PAD - 2, 1),
        (1, PAD + width, PAD + width + 1, -1),
    ):

        def line(at, ex):
            if ex == 0:
                return edges[side, at : at + 1, :]
            return turned[side, 0 if ex == 1 else 1, at : at + 1, :]

        for layer in range(3):
            for row, start, links in (
                (near, 0, tuple(range(19))),
                (far, FAR_ROWS, toward(sign)),
            ):
                into = slice(row, row + 1)
                for k, q in enumerate(links):
                    at, ex = start + 3 * k + layer, LINKS[q][2]
                    moved[q, layer, into, :] = line(at, ex)
                    if ex:
                        kept[q, layer, into, :] = line(at, 0)
                at = start + 3 * len(links) + layer
                for ex in (0, 1, -1):
                    mask[ex % 3, layer, into, :] = line(at, ex)
    face_payload(sol, chem, moved, kept, mask, across, on_chip, (0, width // 8 - 1), True)


def inner_kernel(
    pop,
    sol,
    pore,
    chem,
    moved,
    kept,
    mask,
    edges,
    table,
    flow,
    outer_flow,
    part,
    edge_part,
    edge_chem,
    middle,
    middle_moved,
    buffer,
    sems,
):
    width = pop.shape[2]
    tiles = width // 8
    shifted, plain, masks = readers(moved, kept, mask)
    zero8 = jnp.zeros((8, LX), jnp.float32)
    zero1 = jnp.zeros((1, LX), jnp.float32)

    def pull(layer, row, count, zero):
        return [
            streamed(q, layer, row, count, shifted, plain, masks)
            if 0 <= layer - LINKS[q][0] <= 2
            else zero
            for q in range(19)
        ]

    copies = []
    for layer in (1, 0, 2):
        for t in range(tiles):
            row, rows = PAD + 8 * t, slice(8 * t, 8 * t + 8)
            f = pull(layer, row, 8, zero8)
            rock = pore[layer, rows, :] == 0
            for q in range(19):
                if 0 <= layer - LINKS[q][0] <= 2:
                    v = jnp.where(rock, pop[q, layer, rows, :], f[q])
                    if layer == 1:
                        buffer[q, rows, :] = v
                    else:
                        outer_flow[q, layer // 2, rows, :] = v
            density, mz, my, mx = sums(f)
            if layer != 1:
                for k, v in enumerate((density, mz, my, mx)):
                    part[layer // 2, k, rows, :] = v
                continue
            relaxed = relax_solute(
                [sol[q, layer, rows, :] for q in range(7)],
                chem[0, layer, rows, :],
                chem[1, layer, rows, :],
                jnp.where(rock, 0.0, 1.0 / density),
                (mz, my, mx),
            )
            into = slice(row, row + 8)
            for q in range(7):
                middle[q, into, :] = relaxed[q]
            middle_moved[0, rows, :] = rolled(relaxed[5], 1)
            middle_moved[1, rows, :] = rolled(relaxed[6], -1)
            if t + 1 in (tiles // 2, tiles):
                half = len(copies)
                part_rows = pl.ds(half * (tiles // 2) * 8, (t + 1) * 8 - half * (tiles // 2) * 8)
                copies.append(
                    pltpu.make_async_copy(
                        buffer.at[:, part_rows, :], flow.at[:, 1, part_rows, :], sems.at[half]
                    )
                )
                copies[-1].start()
    for side, row, link, sign in ((0, PAD - 1, 3, 1.0), (1, PAD + width, 4, -1.0)):
        w = W7[link]
        for layer in range(3):
            kind, mineral, total, own = (
                edges[side, 3 * k + layer : 3 * k + layer + 1, :] for k in range(19, 23)
            )
            rate, goal = pick(mineral, table)
            reaction = jnp.where(kind == 2.0, -rate * (total - goal), 0.0)
            base = KEEP_S * own + (w * GAIN_S) * total + w * reaction
            slope = (sign * 4.0 * w * GAIN_S) * total
            density, _, my, _ = sums(pull(layer, row, 1, zero1))
            if layer == 1:
                middle[link, row : row + 1, :] = base + slope * (my / density)
            else:
                at = 2 * side + layer // 2
                edge_part[0, at : at + 1, :] = density
                edge_part[1, at : at + 1, :] = my
                edge_chem[0, at : at + 1, :] = base
                edge_chem[1, at : at + 1, :] = slope
    for copy in copies:
        copy.wait()


def relax_solute(s, total, reaction, inverse, momenta):
    common = (W7[1] * GAIN_S) * total + W7[1] * reaction
    slope = (4.0 * W7[1] * GAIN_S) * total * inverse
    out = [KEEP_S * s[0] + (W7[0] * GAIN_S) * total + W7[0] * reaction]
    for q, m in zip((1, 3, 5), momenta):
        out.append(KEEP_S * s[q] + common + slope * m)
        out.append(KEEP_S * s[q + 1] + common - slope * m)
    return out


def outer_kernel(
    pop,
    sol,
    pore,
    chem,
    moved,
    kept,
    mask,
    part,
    edge_part,
    edge_chem,
    middle,
    middle_moved,
    across,
    on_chip,
    outer_flow,
    flow_in,
    flow,
    solute,
    faces,
    faces_moved,
    cross_s,
    fbuf,
    sbuf,
    sems,
):
    del flow_in
    width = pop.shape[2]
    tiles = width // 8
    own = readers(moved, kept, mask)
    for layer in (0, 2):
        local = [q for q in range(19) if 0 <= layer - LINKS[q][0] <= 2]
        start = 0
        while start < len(local):
            stop = start
            while stop + 1 < len(local) and local[stop + 1] == local[stop] + 1:
                stop += 1
            links = pl.ds(local[start], local[stop] - local[start] + 1)
            pltpu.make_async_copy(
                outer_flow.at[links, layer // 2], flow.at[links, layer], sems.at[0]
            ).start()
            start = stop + 1

    def body(above, below):
        def value(q, layer, row, count):
            ref, links = (below, UP) if layer == -1 else (above, DOWN)
            at = place(links.index(q), links, row, width)
            return ref[at : at + count, :]

        def shifted(q, layer, row, count):
            if 0 <= layer <= 2:
                return own[0](q, layer, row, count)
            return rolled(value(q, layer, row, count), LINKS[q][2])

        def plain(q, layer, row, count):
            if 0 <= layer <= 2:
                return own[1](q, layer, row, count)
            return value(q, layer, row, count)

        def masks(ex, layer, row, count):
            if 0 <= layer <= 2:
                return own[2](ex, layer, row, count)
            at = place(5, UP, row, width)
            return rolled((below if layer == -1 else above)[at : at + count, :], ex)

        def solute_at(q, layer, row, count):
            if layer == 1:
                return middle[q, row : row + count, :]
            return faces[q, layer // 2, row : row + count, :]

        def finish(layer):
            for t in range(tiles):
                row, rows = PAD + 8 * t, slice(8 * t, 8 * t + 8)
                rock = pore[layer, rows, :] == 0
                for q in range(7):
                    ez, ey, ex = LINKS[q]
                    src = layer - ez
                    if src == -1:
                        v = cross_s[0, rows, :]
                    elif src == 3:
                        v = cross_s[1, rows, :]
                    elif ex and layer == 1:
                        v = middle_moved[q - 5, rows, :]
                    elif ex:
                        v = faces_moved[q - 5, layer // 2, rows, :]
                    else:
                        v = solute_at(q, src, row - ey, 8)
                    if q:
                        open_ = masks(ex, src, row - ey, 8) > 0.0
                        v = jnp.where(open_, v, solute_at(REVERSE[q], layer, row, 8))
                    sbuf[q, layer, rows, :] = jnp.where(rock, sol[q, layer, rows, :], v)
            pltpu.make_async_copy(sbuf.at[:, layer], solute.at[:, layer], sems.at[1]).start()

        for side, ref, layer, outside, enter, leave in (
            (0, below, 0, -1, UP, DOWN),
            (1, above, 2, 3, DOWN, UP),
        ):
            sign = 1.0 if side == 0 else -1.0
            for t in range(tiles):
                row, rows = PAD + 8 * t, slice(8 * t, 8 * t + 8)
                rock = pore[layer, rows, :] == 0
                f = {q: streamed(q, layer, row, 8, shifted, plain, masks) for q in enter}
                for k, q in enumerate(enter):
                    fbuf[side, k, rows, :] = jnp.where(rock, pop[q, layer, rows, :], f[q])
                density, mz, my, mx = (part[side, k, rows, :] for k in range(4))
                arrived = add_all(f.values())
                density = density + arrived
                mz = mz + sign * arrived
                for q in enter:
                    _, ey, ex = LINKS[q]
                    if ey:
                        my = my + f[q] if ey == 1 else my - f[q]
                    if ex:
                        mx = mx + f[q] if ex == 1 else mx - f[q]
                relaxed = relax_solute(
                    [sol[q, layer, rows, :] for q in range(7)],
                    chem[0, layer, rows, :],
                    chem[1, layer, rows, :],
                    jnp.where(rock, 0.0, 1.0 / density),
                    (mz, my, mx),
                )
                into = slice(row, row + 8)
                for q in range(7):
                    faces[q, side, into, :] = relaxed[q]
                faces_moved[0, side, rows, :] = rolled(relaxed[5], 1)
                faces_moved[1, side, rows, :] = rolled(relaxed[6], -1)
                back = add_all(
                    streamed(q, outside, row, 8, shifted, plain, masks) for q in leave
                )
                base, partial, weight = (
                    ref[field(k, row, width) : field(k, row, width) + 8, :] for k in range(3)
                )
                cross_s[side, rows, :] = base + weight / (partial + back)
            for k, q in enumerate(enter):
                pltpu.make_async_copy(fbuf.at[side, k], flow.at[q, layer], sems.at[0]).start()
            for end, row, link in ((0, PAD - 1, 3), (1, PAD + width, 4)):
                at = 2 * end + side
                line = slice(at, at + 1)
                f = {q: streamed(q, layer, row, 1, shifted, plain, masks) for q in enter}
                density = edge_part[0, line, :] + add_all(f.values())
                my = edge_part[1, line, :]
                for q in enter:
                    if LINKS[q][1]:
                        my = my + f[q] if LINKS[q][1] == 1 else my - f[q]
                faces[link, side, row : row + 1, :] = edge_chem[0, line, :] + edge_chem[
                    1, line, :
                ] * (my / density)
            finish(layer)
        finish(1)

    by_parity(body, on_chip, across)
    pltpu.make_async_copy(outer_flow, flow.at[:, pl.ds(0, 2)], sems.at[0]).wait()
    pltpu.make_async_copy(sbuf, solute, sems.at[1]).wait()


VMEM = pl.BlockSpec(memory_space=pltpu.VMEM)
ANY = pl.BlockSpec(memory_space=pl.ANY)
HBM = pl.BlockSpec(memory_space=pltpu.HBM)
DMA = pltpu.SemaphoreType.DMA


def call(kernel, operands, specs, outs, scratch=(), aliases=None, flops=1_000_000):
    return pl.pallas_call(
        kernel,
        out_shape=[jax.ShapeDtypeStruct(s, jnp.float32) for s, _ in outs],
        in_specs=list(specs),
        out_specs=[spec for _, spec in outs],
        scratch_shapes=[pltpu.VMEM(s, jnp.float32) if isinstance(s, tuple) else s for s in scratch],
        input_output_aliases=aliases or {},
        compiler_params=pltpu.CompilerParams(vmem_limit_bytes=MAX_VMEM),
        cost_estimate=pl.CostEstimate(flops=flops, bytes_accessed=1_000_000, transcendentals=0),
        name=kernel.__name__,
    )(*operands)


def on_device(populations, solute, pore_mask, mineral_ids, reaction_rates, saturation):
    width = pore_mask.shape[1]
    padded = width + 2 * PAD
    cells = (populations, solute, pore_mask, mineral_ids)
    tables = (reaction_rates, saturation)
    gz, gy = lax.axis_size("gz"), lax.axis_size("gy")
    kinds = reaction_rates.shape
    first, second, table = call(
        pack_edges,
        tuple(pltpu.with_memory_space_constraint(v, pltpu.HBM) for v in cells + tables),
        [HBM] * 6,
        [((EDGE_ROWS, LX), VMEM)] * 2 + [((2 * kinds[0], LX), VMEM)],
        [
            (2, 19, 8, LX),
            (2, 7, 8, LX),
            pltpu.VMEM((2, 8, LX), jnp.int32),
            pltpu.VMEM((2, 8, LX), jnp.int32),
            (2, NEAR, 8, LX),
            pltpu.SMEM(kinds, jnp.float32),
            pltpu.SMEM(kinds, jnp.float32),
            DMA((3,)),
        ],
    )
    def pairs(upward):
        found = []
        for place in range(gz * gy):
            ends = (place, place + 1)
            if ends[1] % gy:
                found.append(ends if upward == (place < gz // 2 * gy) else ends[::-1])
        return found

    first = lax.ppermute(first, ("gz", "gy"), pairs(True))
    second = lax.ppermute(second, ("gz", "gy"), pairs(False))
    rows = 9 * width + 16
    whole = ((19, 3, padded, LX), VMEM)
    masks = ((3, 3, padded, LX), VMEM)
    moved, kept, mask, chem, across, on_chip = call(
        relax_kernel,
        cells + (table,),
        [VMEM] * 5,
        [
            whole,
            whole,
            masks,
            ((2, 3, width, LX), VMEM),
            ((rows, LX), VMEM),
            ((rows, LX), VMEM),
        ],
        flops=6_000_000,
    )
    moved, kept, mask, across, on_chip, edges = call(
        face_kernel,
        (moved, kept, mask, across, on_chip, first, second, solute, chem),
        [VMEM] * 9,
        [
            whole,
            whole,
            masks,
            ((rows, LX), VMEM),
            ((rows, LX), VMEM),
            ((2, EDGE_ROWS, LX), VMEM),
        ],
        [(2, 2, EDGE_ROWS, LX)],
        {k: k for k in range(5)},
    )
    across = lax.ppermute(
        across, "gz", [(i, (i + 1 if i % 2 else i - 1) % gz) for i in range(gz)]
    )
    on_chip = lax.ppermute(on_chip, "gz", [(i, i + 1 - 2 * (i % 2)) for i in range(gz)])
    flow, outer_flow, part, edge_part, edge_chem, middle, middle_moved = call(
        inner_kernel,
        (populations, solute, pore_mask, chem, moved, kept, mask, edges, table),
        [VMEM] * 9,
        [
            (populations.shape, ANY),
            ((19, 2, width, LX), VMEM),
            ((2, 4, width, LX), VMEM),
            ((2, 8, LX), VMEM),
            ((2, 8, LX), VMEM),
            ((7, padded, LX), VMEM),
            ((2, width, LX), VMEM),
        ],
        [(19, width, LX), DMA((2,))],
        flops=6_000_000,
    )
    return tuple(
        call(
            outer_kernel,
            cells[:3]
            + (chem, moved, kept, mask, part, edge_part, edge_chem, middle, middle_moved)
            + (across, on_chip, outer_flow, flow),
            [VMEM] * 15 + [ANY],
            [(populations.shape, ANY), (solute.shape, ANY)],
            [
                (7, 2, padded, LX),
                (2, 2, width, LX),
                (2, width, LX),
                (2, 5, width, LX),
                (7, 3, width, LX),
                DMA((2,)),
            ],
            {15: 0},
        )
    )


def solution(mesh):
    cells = P(None, "gz", "gy", None)
    return jax.shard_map(
        on_device,
        mesh=mesh,
        in_specs=(cells, cells, P("gz", "gy", None), P("gz", "gy", None), P(), P()),
        out_specs=(cells, cells),
        check_vma=False,
    )
```

```python
import functools

import jax
import jax.numpy as jnp
import numpy as np
from jax import lax
from jax.experimental import pallas as pl
from jax.experimental.pallas import tpu as pltpu
from jax.sharding import PartitionSpec as P

LINKS = (
    (0, 0, 0),
    (1, 0, 0),
    (-1, 0, 0),
    (0, 1, 0),
    (0, -1, 0),
    (0, 0, 1),
    (0, 0, -1),
    (1, 1, 0),
    (-1, -1, 0),
    (1, -1, 0),
    (-1, 1, 0),
    (1, 0, 1),
    (-1, 0, -1),
    (1, 0, -1),
    (-1, 0, 1),
    (0, 1, 1),
    (0, -1, -1),
    (0, 1, -1),
    (0, -1, 1),
)
REVERSE = (0, 2, 1, 4, 3, 6, 5, 8, 7, 10, 9, 12, 11, 14, 13, 16, 15, 18, 17)
W19 = (1.0 / 3.0,) + (1.0 / 18.0,) * 6 + (1.0 / 36.0,) * 12
W7 = (0.25,) + (0.125,) * 6
UP = tuple(q for q in range(19) if LINKS[q][0] == 1)
DOWN = tuple(q for q in range(19) if LINKS[q][0] == -1)
KEEP = 1.0 - 1.0 / 1.25
GAIN = 1.0 / 1.25
KEEP_S = 1.0 - 1.0 / 1.4
GAIN_S = 1.0 / 1.4
LX = 128
PAD = 8
MAX_VMEM = 12 * 1024 * 1024
NEAR = 23
FAR_ROWS = 3 * NEAR
EDGE_ROWS = 88


def relax(p):
    d = {q: p[q] - p[q + 1] for q in range(1, 19, 2)}
    s = {q: p[q] + p[q + 1] for q in range(1, 19, 2)}
    density = p[0] + (
        ((s[1] + s[3]) + (s[5] + s[7])) + ((s[9] + s[11]) + (s[13] + s[15])) + s[17]
    )
    mz = (d[1] + d[7]) + (d[9] + d[11]) + d[13]
    my = (d[3] + d[7]) + (d[15] + d[17]) - d[9]
    mx = (d[5] + d[11]) + (d[15] - d[13]) - d[17]
    inverse = 1.0 / density
    uz, uy, ux = mz * inverse, my * inverse, mx * inverse
    rest = 1.0 - 1.5 * (uz * uz + uy * uy + ux * ux)
    out = [None] * 19
    scaled = {w: density * (GAIN * w) for w in set(W19)}
    out[0] = KEEP * p[0] + scaled[W19[0]] * rest
    along = {
        1: uz,
        3: uy,
        5: ux,
        7: uz + uy,
        9: uz - uy,
        11: uz + ux,
        13: uz - ux,
        15: uy + ux,
        17: uy - ux,
    }
    for q, e in along.items():
        w = scaled[W19[q]]
        even = w * (rest + 4.5 * (e * e))
        odd = w * (3.0 * e)
        out[q] = KEEP * p[q] + (even + odd)
        out[q + 1] = KEEP * p[q + 1] + (even - odd)
    return out


def pick(ids, table):
    kinds = table.shape[0] // 2
    rate, goal = table[0:1, :], table[kinds : kinds + 1, :]
    for k in range(1, kinds):
        rate = jnp.where(ids == k, table[k : k + 1, :], rate)
        goal = jnp.where(ids == k, table[kinds + k : kinds + k + 1, :], goal)
    return rate, goal


def solute_terms(s, pore, ids, table):
    total = ((s[0] + s[1]) + (s[2] + s[3])) + ((s[4] + s[5]) + s[6])
    rate, goal = pick(ids, table)
    return total, jnp.where(pore == 2, -rate * (total - goal), 0.0)


def rolled(value, shift):
    return value if shift == 0 else pltpu.roll(value, shift % LX, axis=1)


def sums(f):
    d = {q: f[q] - f[q + 1] for q in range(1, 19, 2)}
    s = {q: f[q] + f[q + 1] for q in range(1, 19, 2)}
    density = f[0] + (
        ((s[1] + s[3]) + (s[5] + s[7])) + ((s[9] + s[11]) + (s[13] + s[15])) + s[17]
    )
    mz = (d[1] + d[7]) + (d[9] + d[11]) + d[13]
    my = (d[3] + d[7]) + (d[15] + d[17]) - d[9]
    mx = (d[5] + d[11]) + (d[15] - d[13]) - d[17]
    return density, mz, my, mx


def add_all(values):
    values = list(values)
    while len(values) > 1:
        values = [
            values[i] + values[i + 1] if i + 1 < len(values) else values[i]
            for i in range(0, len(values), 2)
        ]
    return values[0]


def toward(sign):
    return tuple(q for q in range(19) if LINKS[q][1] == sign)


def either(condition, when_true, when_false):
    pl.when(condition)(when_true)
    pl.when(jnp.logical_not(condition))(when_false)


def upper_half():
    return lax.axis_index("gz") >= lax.axis_size("gz") // 2


def by_parity(body, first, second):
    even = lax.rem(lax.axis_index("gz"), 2) == 0
    either(even, lambda: body(first, second), lambda: body(second, first))


def pack_edges(
    pop,
    sol,
    pore,
    ids,
    rates,
    target,
    first,
    second,
    table,
    epop,
    esol,
    epore,
    eids,
    erel,
    srates,
    starget,
    sems,
):
    width = pop.shape[2]
    for side, start in ((0, width - 2), (1, 0)):
        rows = pl.ds(start, 2)
        for layer in range(3):
            into = pl.ds(2 * layer, 2)
            for src, dst in (
                (pop.at[:, layer, rows, :], epop.at[side, :, into, :]),
                (sol.at[:, layer, rows, :], esol.at[side, :, into, :]),
                (pore.at[layer, rows, :], epore.at[side, into, :]),
                (ids.at[layer, rows, :], eids.at[side, into, :]),
            ):
                pltpu.make_async_copy(src, dst, sems.at[0]).start()
    constants = [
        pltpu.make_async_copy(rates, srates, sems.at[1]),
        pltpu.make_async_copy(target, starget, sems.at[2]),
    ]
    for copy in constants:
        copy.start()
    every = erel.at[:, pl.ds(0, 21)]
    pltpu.make_async_copy(every, every, sems.at[0]).wait()
    for copy in constants:
        copy.wait()
    for side, link in ((0, 3), (1, 4)):
        rel = relax([epop[side, q] for q in range(19)])
        for q in range(19):
            erel[side, q] = rel[q]
        erel[side, 19] = epore[side].astype(jnp.float32)
        erel[side, 20] = eids[side].astype(jnp.float32)
        erel[side, 21] = add_all(esol[side, q] for q in range(7))
        erel[side, 22] = esol[side, link]

    def emit(up, down):
        for side, out, near, far, sign in ((0, up, 1, 0, 1), (1, down, 0, 1, -1)):
            for layer in range(3):
                row = 2 * layer + near
                for k in range(NEAR):
                    at = 3 * k + layer
                    out[at : at + 1, :] = erel[side, k, row : row + 1, :]
                row = 2 * layer + far
                for k, q in enumerate(toward(sign) + (19,)):
                    at = FAR_ROWS + 3 * k + layer
                    out[at : at + 1, :] = erel[side, q, row : row + 1, :]
            out[EDGE_ROWS - 1 : EDGE_ROWS, :] = jnp.zeros((1, LX), jnp.float32)

    either(upper_half(), lambda: emit(second, first), lambda: emit(first, second))
    kinds = srates.shape[0]
    for k in range(kinds):
        for at, ref in ((k, srates), (k + kinds, starget)):
            table[at : at + 1, :] = jnp.full((1, LX), ref[k], jnp.float32)


def place(k, links, row, width):
    if k == 5:
        return 5 * (width + 2) + row - (PAD - 2)
    return k * (width + 2) + row - (PAD - 1 - LINKS[links[k]][1])


def field(k, row, width):
    return 6 * width + 14 + k * width + row - PAD


def face_payload(sol, chem, moved, kept, mask, across, on_chip, tiles, at_edges):
    width = sol.shape[2]
    shifted, plain, masks = readers(moved, kept, mask)

    def emit(up, down):
        for out, layer, cross, link in ((up, 2, UP, 1), (down, 0, DOWN, 2)):
            w = W7[link]
            for t in tiles:
                row, rows = PAD + 8 * t, slice(8 * t, 8 * t + 8)
                get = functools.partial(
                    streamed,
                    layer=layer,
                    row=row,
                    count=8,
                    shifted=shifted,
                    plain=plain,
                    masks=masks,
                )
                away = add_all(get(q) for q in cross)
                level = add_all(get(q) for q in range(19) if LINKS[q][0] == 0)
                partial = level + away
                total, reaction = chem[0, layer, rows, :], chem[1, layer, rows, :]
                slope = (4.0 * w * GAIN_S) * total
                base = KEEP_S * sol[link, layer, rows, :] + (w * GAIN_S) * total + w * reaction
                for k, v in enumerate((base - slope, partial, slope * (partial + away))):
                    at = field(k, row, width)
                    out[at : at + 8, :] = v
            for k in range(6):
                ey = LINKS[cross[k]][1] if k < 5 else 0
                extra = 2 if k == 5 else 1
                below, above = extra + ey, extra - ey
                pieces = [(PAD + 8 * t, 8) for t in range(width // 8)]
                if at_edges:
                    pieces = [(PAD - below, below), (PAD + width, above)]
                for row, count in pieces:
                    if count:
                        at = place(k, cross, row, width)
                        v = plain(cross[k], layer, row, count) if k < 5 else masks(0, layer, row, count)
                        out[at : at + count, :] = v

    by_parity(emit, on_chip, across)


def relax_kernel(pop, sol, pore, ids, table, moved, kept, mask, chem, across, on_chip):
    width = pop.shape[2]
    for layer in range(3):
        for t in range(width // 8):
            rows, into = slice(8 * t, 8 * t + 8), slice(PAD + 8 * t, PAD + 8 * t + 8)
            out = relax([pop[q, layer, rows, :] for q in range(19)])
            for q in range(19):
                ex = LINKS[q][2]
                moved[q, layer, into, :] = rolled(out[q], ex)
                if ex:
                    kept[q, layer, into, :] = out[q]
            kind = pore[layer, rows, :]
            m = jnp.where(kind > 0, 1.0, 0.0)
            for ex in (0, 1, -1):
                mask[ex % 3, layer, into, :] = rolled(m, ex)
            s = [sol[q, layer, rows, :] for q in range(7)]
            total, reaction = solute_terms(s, kind, ids[layer, rows, :], table)
            chem[0, layer, rows, :] = total
            chem[1, layer, rows, :] = reaction
    face_payload(
        sol, chem, moved, kept, mask, across, on_chip, range(1, width // 8 - 1), False
    )


def streamed(q, layer, row, count, shifted, plain, masks):
    ez, ey, ex = LINKS[q]
    value = shifted(q, layer - ez, row - ey, count)
    if q == 0:
        return value
    open_ = masks(ex, layer - ez, row - ey, count) > 0.0
    return jnp.where(open_, value, plain(REVERSE[q], layer, row, count))


def readers(moved, kept, mask):
    def shifted(q, layer, row, count):
        return moved[q, layer, row : row + count, :]

    def plain(q, layer, row, count):
        return (kept if LINKS[q][2] else moved)[q, layer, row : row + count, :]

    def masks(ex, layer, row, count):
        return mask[ex % 3, layer, row : row + count, :]

    return shifted, plain, masks


def face_kernel(
    moved_in,
    kept_in,
    mask_in,
    across_in,
    on_chip_in,
    first,
    second,
    sol,
    chem,
    moved,
    kept,
    mask,
    across,
    on_chip,
    edges,
    turned,
):
    del moved_in, kept_in, mask_in, across_in, on_chip_in
    width = sol.shape[2]
    upper = upper_half()
    for t in range(EDGE_ROWS // 8):
        rows = slice(8 * t, 8 * t + 8)
        for side, v in (
            (0, jnp.where(upper, second[rows, :], first[rows, :])),
            (1, jnp.where(upper, first[rows, :], second[rows, :])),
        ):
            edges[side, rows, :] = v
            turned[side, 0, rows, :] = rolled(v, 1)
            turned[side, 1, rows, :] = rolled(v, -1)
    for side, near, far, sign in (
        (0, PAD - 1, PAD - 2, 1),
        (1, PAD + width, PAD + width + 1, -1),
    ):

        def line(at, ex):
            if ex == 0:
                return edges[side, at : at + 1, :]
            return turned[side, 0 if ex == 1 else 1, at : at + 1, :]

        for layer in range(3):
            for row, start, links in (
                (near, 0, tuple(range(19))),
                (far, FAR_ROWS, toward(sign)),
            ):
                into = slice(row, row + 1)
                for k, q in enumerate(links):
                    at, ex = start + 3 * k + layer, LINKS[q][2]
                    moved[q, layer, into, :] = line(at, ex)
                    if ex:
                        kept[q, layer, into, :] = line(at, 0)
                at = start + 3 * len(links) + layer
                for ex in (0, 1, -1):
                    mask[ex % 3, layer, into, :] = line(at, ex)
    face_payload(sol, chem, moved, kept, mask, across, on_chip, (0, width // 8 - 1), True)


def inner_kernel(
    pop,
    sol,
    pore,
    chem,
    moved,
    kept,
    mask,
    edges,
    table,
    flow,
    outer_flow,
    part,
    edge_part,
    edge_chem,
    middle,
    middle_moved,
    level,
    buffer,
    sems,
):
    width = pop.shape[2]
    tiles = width // 8
    shifted, plain, masks = readers(moved, kept, mask)
    zero8 = jnp.zeros((8, LX), jnp.float32)
    zero1 = jnp.zeros((1, LX), jnp.float32)

    def pull(layer, row, count, zero):
        return [
            streamed(q, layer, row, count, shifted, plain, masks)
            if 0 <= layer - LINKS[q][0] <= 2
            else zero
            for q in range(19)
        ]

    copies = []
    for layer in (1, 0, 2):
        for t in range(tiles):
            row, rows = PAD + 8 * t, slice(8 * t, 8 * t + 8)
            f = pull(layer, row, 8, zero8)
            rock = pore[layer, rows, :] == 0
            for q in range(19):
                if 0 <= layer - LINKS[q][0] <= 2:
                    v = jnp.where(rock, pop[q, layer, rows, :], f[q])
                    if layer == 1:
                        buffer[q, rows, :] = v
                    else:
                        outer_flow[q, layer // 2, rows, :] = v
            density, mz, my, mx = sums(f)
            if layer != 1:
                for k, v in enumerate((density, mz, my, mx)):
                    part[layer // 2, k, rows, :] = v
                continue
            relaxed = relax_solute(
                [sol[q, layer, rows, :] for q in range(7)],
                chem[0, layer, rows, :],
                chem[1, layer, rows, :],
                jnp.where(rock, 0.0, 1.0 / density),
                (mz, my, mx),
            )
            into = slice(row, row + 8)
            for q in range(7):
                middle[q, into, :] = relaxed[q]
            middle_moved[0, rows, :] = rolled(relaxed[5], 1)
            middle_moved[1, rows, :] = rolled(relaxed[6], -1)
            if t + 1 in (tiles // 2, tiles):
                half = len(copies)
                part_rows = pl.ds(half * (tiles // 2) * 8, (t + 1) * 8 - half * (tiles // 2) * 8)
                copies.append(
                    pltpu.make_async_copy(
                        buffer.at[:, part_rows, :], flow.at[:, 1, part_rows, :], sems.at[half]
                    )
                )
                copies[-1].start()
    for side, row, link, sign in ((0, PAD - 1, 3, 1.0), (1, PAD + width, 4, -1.0)):
        w = W7[link]
        for layer in range(3):
            kind, mineral, total, own = (
                edges[side, 3 * k + layer : 3 * k + layer + 1, :] for k in range(19, 23)
            )
            rate, goal = pick(mineral, table)
            reaction = jnp.where(kind == 2.0, -rate * (total - goal), 0.0)
            base = KEEP_S * own + (w * GAIN_S) * total + w * reaction
            slope = (sign * 4.0 * w * GAIN_S) * total
            density, _, my, _ = sums(pull(layer, row, 1, zero1))
            if layer == 1:
                middle[link, row : row + 1, :] = base + slope * (my / density)
            else:
                at = 2 * side + layer // 2
                edge_part[0, at : at + 1, :] = density
                edge_part[1, at : at + 1, :] = my
                edge_chem[0, at : at + 1, :] = base
                edge_chem[1, at : at + 1, :] = slope
    for t in range(tiles):
        row, rows = PAD + 8 * t, slice(8 * t, 8 * t + 8)
        rock = pore[1, rows, :] == 0
        for q in (0, 3, 4, 5, 6):
            _, ey, ex = LINKS[q]
            v = middle_moved[q - 5, rows, :] if ex else middle[q, row - ey : row - ey + 8, :]
            if q:
                open_ = masks(ex, 1, row - ey, 8) > 0.0
                v = jnp.where(open_, v, middle[REVERSE[q], row : row + 8, :])
            level[q, rows, :] = jnp.where(rock, sol[q, 1, rows, :], v)
    for copy in copies:
        copy.wait()


def relax_solute(s, total, reaction, inverse, momenta):
    common = (W7[1] * GAIN_S) * total + W7[1] * reaction
    slope = (4.0 * W7[1] * GAIN_S) * total * inverse
    out = [KEEP_S * s[0] + (W7[0] * GAIN_S) * total + W7[0] * reaction]
    for q, m in zip((1, 3, 5), momenta):
        out.append(KEEP_S * s[q] + common + slope * m)
        out.append(KEEP_S * s[q + 1] + common - slope * m)
    return out


def outer_kernel(
    pop,
    sol,
    pore,
    chem,
    moved,
    kept,
    mask,
    part,
    edge_part,
    edge_chem,
    middle,
    level,
    across,
    on_chip,
    outer_flow,
    flow_in,
    flow,
    solute,
    faces,
    faces_moved,
    cross_s,
    fbuf,
    sbuf,
    sems,
):
    del flow_in
    width = pop.shape[2]
    tiles = width // 8
    own = readers(moved, kept, mask)
    for links in (pl.ds(0, 1), pl.ds(3, 4)):
        pltpu.make_async_copy(level.at[links], solute.at[links, 1], sems.at[1]).start()
    for layer in (0, 2):
        local = [q for q in range(19) if 0 <= layer - LINKS[q][0] <= 2]
        start = 0
        while start < len(local):
            stop = start
            while stop + 1 < len(local) and local[stop + 1] == local[stop] + 1:
                stop += 1
            links = pl.ds(local[start], local[stop] - local[start] + 1)
            pltpu.make_async_copy(
                outer_flow.at[links, layer // 2], flow.at[links, layer], sems.at[0]
            ).start()
            start = stop + 1

    def body(above, below):
        def value(q, layer, row, count):
            ref, links = (below, UP) if layer == -1 else (above, DOWN)
            at = place(links.index(q), links, row, width)
            return ref[at : at + count, :]

        def shifted(q, layer, row, count):
            if 0 <= layer <= 2:
                return own[0](q, layer, row, count)
            return rolled(value(q, layer, row, count), LINKS[q][2])

        def plain(q, layer, row, count):
            if 0 <= layer <= 2:
                return own[1](q, layer, row, count)
            return value(q, layer, row, count)

        def masks(ex, layer, row, count):
            if 0 <= layer <= 2:
                return own[2](ex, layer, row, count)
            at = place(5, UP, row, width)
            return rolled((below if layer == -1 else above)[at : at + count, :], ex)

        def solute_at(q, layer, row, count):
            if layer == 1:
                return middle[q, row : row + count, :]
            return faces[q, layer // 2, row : row + count, :]

        def finish(layer):
            for t in range(tiles):
                row, rows = PAD + 8 * t, slice(8 * t, 8 * t + 8)
                rock = pore[layer, rows, :] == 0
                for q in (1, 2) if layer == 1 else range(7):
                    ez, ey, ex = LINKS[q]
                    src = layer - ez
                    if src == -1:
                        v = cross_s[0, rows, :]
                    elif src == 3:
                        v = cross_s[1, rows, :]
                    elif ex:
                        v = faces_moved[q - 5, layer // 2, rows, :]
                    else:
                        v = solute_at(q, src, row - ey, 8)
                    if q:
                        open_ = masks(ex, src, row - ey, 8) > 0.0
                        v = jnp.where(open_, v, solute_at(REVERSE[q], layer, row, 8))
                    sbuf[q, layer, rows, :] = jnp.where(rock, sol[q, layer, rows, :], v)
            links = pl.ds(1, 2) if layer == 1 else pl.ds(0, 7)
            pltpu.make_async_copy(
                sbuf.at[links, layer], solute.at[links, layer], sems.at[1]
            ).start()

        for side, ref, layer, outside, enter, leave in (
            (0, below, 0, -1, UP, DOWN),
            (1, above, 2, 3, DOWN, UP),
        ):
            sign = 1.0 if side == 0 else -1.0
            for t in range(tiles):
                row, rows = PAD + 8 * t, slice(8 * t, 8 * t + 8)
                rock = pore[layer, rows, :] == 0
                f = {q: streamed(q, layer, row, 8, shifted, plain, masks) for q in enter}
                for k, q in enumerate(enter):
                    fbuf[side, k, rows, :] = jnp.where(rock, pop[q, layer, rows, :], f[q])
                density, mz, my, mx = (part[side, k, rows, :] for k in range(4))
                arrived = add_all(f.values())
                density = density + arrived
                mz = mz + sign * arrived
                for q in enter:
                    _, ey, ex = LINKS[q]
                    if ey:
                        my = my + f[q] if ey == 1 else my - f[q]
                    if ex:
                        mx = mx + f[q] if ex == 1 else mx - f[q]
                relaxed = relax_solute(
                    [sol[q, layer, rows, :] for q in range(7)],
                    chem[0, layer, rows, :],
                    chem[1, layer, rows, :],
                    jnp.where(rock, 0.0, 1.0 / density),
                    (mz, my, mx),
                )
                into = slice(row, row + 8)
                for q in range(7):
                    faces[q, side, into, :] = relaxed[q]
                faces_moved[0, side, rows, :] = rolled(relaxed[5], 1)
                faces_moved[1, side, rows, :] = rolled(relaxed[6], -1)
                back = add_all(
                    streamed(q, outside, row, 8, shifted, plain, masks) for q in leave
                )
                base, partial, weight = (
                    ref[field(k, row, width) : field(k, row, width) + 8, :] for k in range(3)
                )
                cross_s[side, rows, :] = base + weight / (partial + back)
            for k, q in enumerate(enter):
                pltpu.make_async_copy(fbuf.at[side, k], flow.at[q, layer], sems.at[0]).start()
            for end, row, link in ((0, PAD - 1, 3), (1, PAD + width, 4)):
                at = 2 * end + side
                line = slice(at, at + 1)
                f = {q: streamed(q, layer, row, 1, shifted, plain, masks) for q in enter}
                density = edge_part[0, line, :] + add_all(f.values())
                my = edge_part[1, line, :]
                for q in enter:
                    if LINKS[q][1]:
                        my = my + f[q] if LINKS[q][1] == 1 else my - f[q]
                faces[link, side, row : row + 1, :] = edge_chem[0, line, :] + edge_chem[
                    1, line, :
                ] * (my / density)
            finish(layer)
        finish(1)

    by_parity(body, on_chip, across)
    pltpu.make_async_copy(outer_flow, flow.at[:, pl.ds(0, 2)], sems.at[0]).wait()
    pltpu.make_async_copy(sbuf, solute, sems.at[1]).wait()


VMEM = pl.BlockSpec(memory_space=pltpu.VMEM)
ANY = pl.BlockSpec(memory_space=pl.ANY)
HBM = pl.BlockSpec(memory_space=pltpu.HBM)
DMA = pltpu.SemaphoreType.DMA


def call(kernel, operands, specs, outs, scratch=(), aliases=None, flops=1_000_000):
    return pl.pallas_call(
        kernel,
        out_shape=[jax.ShapeDtypeStruct(s, jnp.float32) for s, _ in outs],
        in_specs=list(specs),
        out_specs=[spec for _, spec in outs],
        scratch_shapes=[pltpu.VMEM(s, jnp.float32) if isinstance(s, tuple) else s for s in scratch],
        input_output_aliases=aliases or {},
        compiler_params=pltpu.CompilerParams(vmem_limit_bytes=MAX_VMEM),
        cost_estimate=pl.CostEstimate(flops=flops, bytes_accessed=1_000_000, transcendentals=0),
        name=kernel.__name__,
    )(*operands)


def on_device(populations, solute, pore_mask, mineral_ids, reaction_rates, saturation):
    width = pore_mask.shape[1]
    padded = width + 2 * PAD
    cells = (populations, solute, pore_mask, mineral_ids)
    tables = (reaction_rates, saturation)
    gz, gy = lax.axis_size("gz"), lax.axis_size("gy")
    kinds = reaction_rates.shape
    first, second, table = call(
        pack_edges,
        tuple(pltpu.with_memory_space_constraint(v, pltpu.HBM) for v in cells + tables),
        [HBM] * 6,
        [((EDGE_ROWS, LX), VMEM)] * 2 + [((2 * kinds[0], LX), VMEM)],
        [
            (2, 19, 8, LX),
            (2, 7, 8, LX),
            pltpu.VMEM((2, 8, LX), jnp.int32),
            pltpu.VMEM((2, 8, LX), jnp.int32),
            (2, NEAR, 8, LX),
            pltpu.SMEM(kinds, jnp.float32),
            pltpu.SMEM(kinds, jnp.float32),
            DMA((3,)),
        ],
    )
    def pairs(upward):
        found = []
        for place in range(gz * gy):
            ends = (place, place + 1)
            if ends[1] % gy:
                found.append(ends if upward == (place < gz // 2 * gy) else ends[::-1])
        return found

    first = lax.ppermute(first, ("gz", "gy"), pairs(True))
    second = lax.ppermute(second, ("gz", "gy"), pairs(False))
    rows = 9 * width + 16
    whole = ((19, 3, padded, LX), VMEM)
    masks = ((3, 3, padded, LX), VMEM)
    moved, kept, mask, chem, across, on_chip = call(
        relax_kernel,
        cells + (table,),
        [VMEM] * 5,
        [
            whole,
            whole,
            masks,
            ((2, 3, width, LX), VMEM),
            ((rows, LX), VMEM),
            ((rows, LX), VMEM),
        ],
        flops=6_000_000,
    )
    moved, kept, mask, across, on_chip, edges = call(
        face_kernel,
        (moved, kept, mask, across, on_chip, first, second, solute, chem),
        [VMEM] * 9,
        [
            whole,
            whole,
            masks,
            ((rows, LX), VMEM),
            ((rows, LX), VMEM),
            ((2, EDGE_ROWS, LX), VMEM),
        ],
        [(2, 2, EDGE_ROWS, LX)],
        {k: k for k in range(5)},
    )
    across = lax.ppermute(
        across, "gz", [(i, (i + 1 if i % 2 else i - 1) % gz) for i in range(gz)]
    )
    on_chip = lax.ppermute(on_chip, "gz", [(i, i + 1 - 2 * (i % 2)) for i in range(gz)])
    flow, outer_flow, part, edge_part, edge_chem, middle, _, level = call(
        inner_kernel,
        (populations, solute, pore_mask, chem, moved, kept, mask, edges, table),
        [VMEM] * 9,
        [
            (populations.shape, ANY),
            ((19, 2, width, LX), VMEM),
            ((2, 4, width, LX), VMEM),
            ((2, 8, LX), VMEM),
            ((2, 8, LX), VMEM),
            ((7, padded, LX), VMEM),
            ((2, width, LX), VMEM),
            ((7, width, LX), VMEM),
        ],
        [(19, width, LX), DMA((2,))],
        flops=6_000_000,
    )
    return tuple(
        call(
            outer_kernel,
            cells[:3]
            + (chem, moved, kept, mask, part, edge_part, edge_chem, middle, level)
            + (across, on_chip, outer_flow, flow),
            [VMEM] * 15 + [ANY],
            [(populations.shape, ANY), (solute.shape, ANY)],
            [
                (7, 2, padded, LX),
                (2, 2, width, LX),
                (2, width, LX),
                (2, 5, width, LX),
                (7, 3, width, LX),
                DMA((2,)),
            ],
            {15: 0},
        )
    )


def solution(mesh):
    cells = P(None, "gz", "gy", None)
    return jax.shard_map(
        on_device,
        mesh=mesh,
        in_specs=(cells, cells, P("gz", "gy", None), P("gz", "gy", None), P(), P()),
        out_specs=(cells, cells),
        check_vma=False,
    )
```
